32 devices in a mesh: groups: 2 (over y), seq: 4 (over z), fsdp: 2 (over x), sub: 2 (over core).
Axes of the slice: x: 2, y: 2, z: 4, core: 2. Of those that a mesh axis runs over, the one named last changes fastest.
Arguments:
- tokens: bfloat16 [2048, 8192], P(('groups', 'seq')), parts along dimension 0, may hold values from -400 to 400
- norm_gain: float32 [8192], replicated, may hold values from 0.1 to 1.9
- w_query: bfloat16 [8, 16, 8192], P(('seq', 'sub'), 'fsdp'), may hold values from -0.0625 to 0.0625
- w_key: bfloat16 [8, 16, 8192], P(('seq', 'sub'), 'fsdp'), may hold values from -0.0625 to 0.0625
- w_value: bfloat16 [8, 128, 8192], P(('seq', 'sub'), 'fsdp'), may hold values from -5 to 5
- head_gain: float32 [128], replicated, may hold values from 0.1 to 1.9
- w_out: bfloat16 [8, 128, 8192], P('seq', None, ('fsdp', 'sub')), may hold values from -0.1875 to 0.1875
Outputs:
- mixed: bfloat16 [2048, 8192], P(('groups', 'seq'), ('fsdp', 'sub')), parts along dimension 0
The draws below stay inside these ranges and needn't reach their ends.
There are 2 independent parts, one for each index of `groups`. The reference program is written for one: setup_inputs(seed, part) draws one part's arguments, and reference() takes and returns one part's arrays. A program takes and returns all parts, laid end to end along the dimension named above; an argument that names none is the same for every part. Nothing has to cross between parts.
All inputs are finite; a program needn't handle non-finite values.
Results may differ from the reference program's by a relative error of at most 0.0084.
Values may be sent and summed in bfloat16 or wider, within the bound.
A program may use at most 64 MiB of HBM per device.

```python
import math
import jax
import jax.numpy as jnp
import numpy as np
from jax import lax

D = 8192
HEAD_DIM = 128
FEAT = 16
BLOCK = 512
HEADS = 8
L = 1024


def draw_tokens(key, part):
    subkeys = jax.random.split(jax.random.fold_in(key, 101), 3)
    row_scale = jnp.exp(jax.random.uniform(subkeys[0], (L, 1), jnp.float32, 0.0, math.log(10.0)))
    col_scale = jnp.exp(jax.random.uniform(subkeys[1], (1, D), jnp.float32, 0.0, math.log(10.0)))
    entries = jnp.clip(jax.random.normal(subkeys[2], (L, D), jnp.float32), -4.0, 4.0)
    return (entries * row_scale * col_scale).astype(jnp.bfloat16)


def draw_w_value(key, part):
    subkeys = jax.random.split(jax.random.fold_in(key, 202), 2)
    upward = jnp.arange(HEAD_DIM, dtype=jnp.float32)[None, :, None] / (HEAD_DIM - 1.0)
    jitter = jax.random.uniform(subkeys[0], (HEADS, HEAD_DIM, 1), jnp.float32, 0.0, 1.0)
    exponent = 0.5 * upward + 0.5 * jitter
    entries = jnp.clip(jax.random.normal(subkeys[1], (HEADS, HEAD_DIM, D), jnp.float32), -4.0, 4.0)
    factor = jnp.power(10.0, exponent) / math.sqrt(D)
    return (entries * factor).astype(jnp.bfloat16)


def levels(key, extent, cuts, low, top_value):
    gain, own = 1.0, jax.random.fold_in(key, 6)
    for position, parts in cuts:
        draws = jnp.exp(jax.random.uniform(jax.random.fold_in(own, position), (parts,), jnp.float32, low / len(cuts), top_value / len(cuts)))
        gain = gain * jnp.repeat(draws, extent[position] // parts).reshape([-1 if axis == position else 1 for axis in range(len(extent))])
    return gain


def centred(own_key, dims, width, limit, cuts=(), kind=jnp.bfloat16):
    drawn = jax.random.normal(own_key, dims, jnp.float32) * width
    if len(cuts) > 0:
        drawn = levels(own_key, dims, cuts, -0.22, 0.18) * drawn
    return jnp.clip(drawn, min=-limit, max=limit).astype(kind)


def setup_inputs(seed: int = 0, part: int = 0) -> dict:
    key_list = jax.random.split(jax.random.key(seed), 8)
    own_keys = jax.random.split(jax.random.fold_in(key_list[7], part), 8)
    tokens = draw_tokens(jax.random.fold_in(jax.random.fold_in(key_list[7], part), 71), part)
    norm_gain = jnp.clip(1.0 + 0.18 * jax.random.normal(key_list[1], (D,), jnp.float32), 0.1, 1.9)
    w_query = centred(key_list[2], (HEADS, FEAT, D), D ** -0.5, 0.0625, ((0, 8), (1, 2)))
    w_key = centred(key_list[3], (HEADS, FEAT, D), D ** -0.5, 0.0625, ((0, 8), (1, 2)))
    w_value = draw_w_value(jax.random.fold_in(key_list[7], 71), part)
    head_gain = jnp.clip(1.0 + 0.18 * jax.random.normal(key_list[5], (HEAD_DIM,), jnp.float32), 0.1, 1.9)
    w_out = centred(key_list[6], (HEADS, HEAD_DIM, D), (HEADS * HEAD_DIM) ** -0.5, 0.1875, ((0, 4), (2, 4)))
    return dict(tokens=tokens, norm_gain=norm_gain, w_query=w_query, w_key=w_key, w_value=w_value, head_gain=head_gain, w_out=w_out)


def taylor_last(vectors):
    feature_count = vectors.shape[-1]
    first_row, second_row = np.triu_indices(feature_count, 1)
    cross_terms = vectors[..., first_row] * vectors[..., second_row] / 4.0
    squares = vectors * vectors / (4.0 * math.sqrt(2.0))
    leading = jnp.ones(vectors.shape[:-1] + (1,), jnp.float32)
    return jnp.concatenate([leading, vectors / 2.0, cross_terms, squares], -1)

def reference(tokens, norm_gain, w_query, w_key, w_value, head_gain, w_out):
    inputs = tokens.astype(jnp.float32)
    meansq = lax.optimization_barrier(jnp.mean(inputs * inputs, axis=-1, keepdims=True))
    normed = (inputs * lax.rsqrt(meansq + 1e-05) * norm_gain).astype(jnp.bfloat16)
    length = tokens.shape[0]

    def project(weight):
        flattened = weight.reshape(-1, weight.shape[-1])
        result = jnp.dot(normed, flattened.T, preferred_element_type=jnp.float32)
        result = result.astype(jnp.bfloat16).reshape(length, weight.shape[0], weight.shape[1])
        return jnp.transpose(result, (1, 0, 2))
    queries = project(w_query)
    key_vectors = project(w_key)
    values_all = project(w_value)
    nblocks = length // BLOCK
    position_t = jnp.arange(BLOCK, dtype=jnp.int32)[:, None]
    position_j = jnp.arange(BLOCK, dtype=jnp.int32)[None, :]
    causal = position_j <= position_t

    def one_head(operands):
        head_query, head_key, head_value = operands
        query_feats = taylor_last(head_query.astype(jnp.float32)).astype(jnp.bfloat16)
        key_feats = taylor_last(head_key.astype(jnp.float32)).astype(jnp.bfloat16)
        key_blocks = key_feats.astype(jnp.float32).reshape(nblocks, BLOCK, -1)
        value_blocks = head_value.astype(jnp.float32).reshape(nblocks, BLOCK, -1)
        contrib = jnp.einsum('bjf,bje->bfe', key_blocks, value_blocks)
        prefix = jnp.concatenate([jnp.zeros_like(contrib[:1]), jnp.cumsum(contrib[:-1], axis=0)], 0)
        prior_state = prefix.astype(jnp.bfloat16)
        query_blocks = head_query.astype(jnp.float32).reshape(nblocks, BLOCK, -1)
        raw_keys = head_key.astype(jnp.float32).reshape(nblocks, BLOCK, -1)
        scores = jnp.einsum('btf,bjf->btj', query_blocks, raw_keys)
        kernel = 1.0 + scores / 4.0 + scores * scores / 32.0
        weight = jnp.where(causal[None], kernel, 0.0).astype(jnp.bfloat16)
        local_part = jnp.einsum('btj,bje->bte', weight.astype(jnp.float32), value_blocks)
        feat_blocks = query_feats.astype(jnp.float32).reshape(nblocks, BLOCK, -1)
        carried = jnp.einsum('btf,bfe->bte', feat_blocks, prior_state.astype(jnp.float32))
        return (local_part + carried).reshape(length, -1).astype(jnp.bfloat16)
    numerator = lax.map(one_head, (queries, key_vectors, values_all))
    widened = numerator.astype(jnp.float32)
    meansq_out = lax.optimization_barrier(jnp.mean(widened * widened, axis=-1, keepdims=True))
    attended = (widened * lax.rsqrt(meansq_out + 1e-06) * head_gain).astype(jnp.bfloat16)
    flat_att = jnp.transpose(attended, (1, 0, 2)).reshape(length, -1)
    out_rows = w_out.reshape(-1, w_out.shape[-1])
    return jnp.dot(flat_att, out_rows, preferred_element_type=jnp.float32).astype(jnp.bfloat16)
```

```python
import functools

import jax
import jax.numpy as jnp
from jax import lax
from jax.experimental import pallas as pl
from jax.experimental.pallas import tpu as pltpu
from jax.sharding import PartitionSpec as P

MESH = pl.DeviceIdType.MESH
F32 = jnp.float32
BF16 = jnp.bfloat16


def kernel(
    n,
    nf,
    ns,
    pieces,
    out_pieces,
    w_count,
    tok_hbm,
    gain_ref,
    head_gain_ref,
    wo_hbm,
    *rest,
):
    kernel_body(
        n, nf, ns, pieces, out_pieces, tok_hbm, gain_ref, head_gain_ref, wo_hbm,
        rest[:w_count], *rest[w_count:]
    )


def kernel_body(
    n,
    nf,
    ns,
    pieces,
    out_pieces,
    tok_hbm,
    gain_ref,
    head_gain_ref,
    wo_hbm,
    w_hbm,
    out_ref,
    tok_ref,
    w_ref,
    wo_ref,
    load_sem,
    normed,
    wbuf,
    wobuf,
    qk_send,
    v_send,
    qk_all,
    v_all,
    q_full,
    k_full,
    num_send,
    num_all,
    attended,
    total,
    w_zrecv,
    w_yrecv,
    w_right,
    w_left,
    w_across,
    o_zrecv,
    o_yrecv,
    o_right,
    o_left,
    o_across,
    qk_ssem,
    qk_rsem,
    v_ssem,
    v_rsem,
    num_ssem,
    num_rsem,
    sib_ssem,
    sib_rsem,
):
    group = lax.axis_index("groups")
    me = lax.axis_index("seq")
    my_f = lax.axis_index("fsdp")
    my_s = lax.axis_index("sub")
    tokens, width = tok_ref.shape

    loads = []
    row = 0
    for k, source in enumerate(w_hbm):
        size = source.shape[0]
        target = w_ref.at[pl.ds(row, size)] if len(w_hbm) > 1 else w_ref
        loads.append(pltpu.make_async_copy(source, target, load_sem.at[k]))
        row += size
    tok_load = pltpu.make_async_copy(tok_hbm, tok_ref, load_sem.at[len(w_hbm)])
    wo_load = pltpu.make_async_copy(wo_hbm, wo_ref, load_sem.at[len(w_hbm) + 1])
    for load in loads + [tok_load, wo_load]:
        load.start()

    peers = [
        {"seq": lax.rem(me + dz, n), "fsdp": lax.rem(my_f + df, nf)}
        for dz in range(n)
        for df in range(nf)
        if dz or df
    ]
    peers += [
        {"fsdp": lax.rem(my_f + df, nf), "sub": lax.rem(my_s + ds, ns)}
        for df in range(nf)
        for ds in range(1, ns)
    ]
    peers += [{"groups": 1 - group}]
    barrier = pltpu.get_barrier_semaphore()
    for peer in peers:
        pl.semaphore_signal(barrier, inc=1, device_id=peer, device_id_type=MESH)
    pl.semaphore_wait(barrier, len(peers))
    for load in loads:
        load.wait()
    span = width // (2 * pieces)
    qk_rows = qk_all.shape[2]
    half_rows = qk_rows // 2

    def own_w(c):
        start = pl.multiple_of((group * pieces + c) * span, span)
        return w_ref.at[:, pl.ds(start, span)]

    def own_o(c):
        return wo_ref.at[group, c]

    class Stream:
        def __init__(self, own, buf, count, zrecv, yrecv, right, left, across):
            self.own, self.buf, self.count = own, buf, count
            self.zrecv, self.yrecv = zrecv, yrecv
            self.right_sem, self.left_sem, self.across_sem = right, left, across

        def along(self, o, c, sems, target, own):
            slot = self.buf.at[o, group, c]
            return pltpu.make_async_remote_copy(
                src_ref=self.own(c) if own else slot,
                dst_ref=slot,
                send_sem=sems.at[o, c],
                recv_sem=self.zrecv.at[o, c],
                device_id={"seq": target},
                device_id_type=MESH,
            )

        def right(self, o, c, own=False):
            return self.along(o, c, self.right_sem, me + 1, own)

        def left(self, o, c, own=False):
            return self.along(o, c, self.left_sem, me - 1, own)

        def across(self, o, c, half):
            slot = self.buf.at[o, half, c]
            return pltpu.make_async_remote_copy(
                src_ref=slot,
                dst_ref=slot,
                send_sem=self.across_sem.at[o, c],
                recv_sem=self.yrecv.at[o, c],
                device_id={"groups": 1 - group},
                device_id_type=MESH,
            )

        def begin(self):
            for c in range(self.count):

                @pl.when(me + 1 < n)
                def _():
                    self.right(me, c, True).start()

                @pl.when(me >= 1)
                def _():
                    self.left(me, c, True).start()

        def relay(self, r, between=None):
            for c in range(self.count):
                if between is not None and c == self.count // 2:
                    between()

                @pl.when(me >= r)
                def _():
                    o = me - r
                    self.right(o, c).wait_recv()

                    @pl.when(me + 1 < n)
                    def _():
                        self.right(o, c).start()

                    self.across(o, c, group).start()

                @pl.when(me + r < n)
                def _():
                    o = me + r
                    self.left(o, c).wait_recv()

                    @pl.when(me >= 1)
                    def _():
                        self.left(o, c).start()

                    self.across(o, c, group).start()

        def arrive(self, o):
            for c in range(self.count):
                self.across(o, c, 1 - group).wait_recv()

        def finish(self):
            for r in range(n):
                for c in range(self.count):

                    @pl.when((me >= r) & (me + 1 < n))
                    def _():
                        self.right(me - r, c, r == 0).wait_send()

                    @pl.when((me + r < n) & (me >= 1))
                    def _():
                        self.left(me + r, c, r == 0).wait_send()

                    if r > 0:

                        @pl.when(me >= r)
                        def _():
                            self.across(me - r, c, group).wait_send()

                        @pl.when(me + r < n)
                        def _():
                            self.across(me + r, c, group).wait_send()

    w_stream = Stream(own_w, wbuf, pieces, w_zrecv, w_yrecv, w_right, w_left, w_across)
    o_stream = Stream(own_o, wobuf, out_pieces, o_zrecv, o_yrecv, o_right, o_left, o_across)

    w_stream.begin()
    wo_load.wait()
    at_end = (me == 0) | (me == n - 1)

    @pl.when(at_end)
    def _():
        o_stream.begin()

    tok_load.wait()

    row_step = 16

    def norm_rows(i, carry):
        rows = pl.ds(pl.multiple_of(i * row_step, row_step), row_step)
        sumsq = jnp.zeros((row_step, 1), F32)
        for c in range(2 * pieces):
            part = tok_ref[rows, c * span : (c + 1) * span].astype(F32)
            sumsq = sumsq + jnp.sum(part * part, axis=1, keepdims=True)
        scale = lax.rsqrt(sumsq / width + 1e-05)
        for c in range(2 * pieces):
            cols = slice(c * span, (c + 1) * span)
            part = tok_ref[rows, cols].astype(F32)
            normed[c, rows, :] = (part * scale * gain_ref[:, cols]).astype(BF16)
        return carry

    lax.fori_loop(0, tokens // row_step, norm_rows, 0)

    def contract(weights, acts):
        return lax.dot_general(weights, acts, (((1,), (1,)), ((), ())), preferred_element_type=F32)

    def qk_copy(o, source, other_f, token_block, f_from):
        return pltpu.make_async_remote_copy(
            src_ref=source,
            dst_ref=qk_all.at[token_block, f_from],
            send_sem=qk_ssem.at[o, other_f],
            recv_sem=qk_rsem.at[token_block, f_from],
            device_id={"seq": o, "fsdp": other_f},
            device_id_type=MESH,
        )

    def v_copy(o, token_block):
        return pltpu.make_async_remote_copy(
            src_ref=v_send.at[o],
            dst_ref=v_all.at[token_block],
            send_sem=v_ssem.at[o],
            recv_sem=v_rsem.at[token_block],
            device_id={"seq": o},
            device_id_type=MESH,
        )

    def project_own():
        acc = jnp.zeros((w_ref.shape[0], tokens), F32)
        for c in range(2 * pieces):
            acc = acc + contract(w_ref[:, c * span : (c + 1) * span], normed[c])
        qk_all[me, my_f] = acc[:qk_rows].astype(BF16)
        v_all[me] = acc[qk_rows:].astype(BF16)
        for df in range(1, nf):
            other = lax.rem(my_f + df, nf)
            qk_copy(me, qk_all.at[me, my_f], other, me, my_f).start()

    def project(o):
        def body(c, acc):
            return acc + contract(wbuf[o, c // pieces, c % pieces], normed[c])

        acc = lax.fori_loop(0, 2 * pieces, body, jnp.zeros((w_ref.shape[0], tokens), F32))
        qk_send[o] = acc[:qk_rows].astype(BF16)
        v_send[o] = acc[qk_rows:].astype(BF16)
        for df in range(nf):
            qk_copy(o, qk_send.at[o], lax.rem(my_f + df, nf), me, my_f).start()
        v_copy(o, me).start()

    def both(r, action):
        @pl.when(me >= r)
        def _():
            action(me - r)

        @pl.when(me + r < n)
        def _():
            action(me + r)

    def take(o):
        w_stream.arrive(o)
        project(o)

    project_own()
    for r in range(1, n):
        if r == n - 1:

            @pl.when(jnp.logical_not(at_end))
            def _():
                o_stream.begin()

        w_stream.relay(r, functools.partial(both, r - 1, take) if r > 1 else None)

    o_stream.relay(1, functools.partial(both, n - 1, take))

    def gather_heads():
        for d in range(1, n):
            t = lax.rem(me + d, n)
            v_copy(me, t).wait_recv()
            for df in range(nf):
                qk_copy(me, qk_all.at[t, df], 0, t, df).wait_recv()
        for df in range(1, nf):
            other = lax.rem(my_f + df, nf)
            qk_copy(me, qk_all.at[me, other], other, me, other).wait_recv()

        for t in range(n):
            parts = [qk_all[t, f].astype(F32) for f in range(nf)]
            q_full[t] = jnp.concatenate([p[:half_rows] for p in parts], 0).astype(BF16)
            k_full[t] = jnp.concatenate([p[half_rows:] for p in parts], 0).astype(BF16)

    channels = v_all.shape[1]
    key_pos = lax.broadcasted_iota(jnp.int32, (tokens, tokens), 0)
    query_pos = lax.broadcasted_iota(jnp.int32, (tokens, tokens), 1)

    def numerator(t):
        queries = q_full[t]

        def body(j, acc):
            scores = lax.dot_general(
                k_full[j], queries, (((0,), (0,)), ((), ())), preferred_element_type=F32
            )
            value = 1.0 + scores * 0.25 + scores * scores * 0.03125
            weight = jnp.where(key_pos + (j - t) * tokens <= query_pos, value, 0.0).astype(BF16)
            return acc + jnp.dot(v_all[j], weight, preferred_element_type=F32)

        acc = lax.fori_loop(0, t + 1, body, jnp.zeros((channels, tokens), F32))
        return acc.astype(BF16)

    def num_copy(t, head_block):
        return pltpu.make_async_remote_copy(
            src_ref=num_send.at[t],
            dst_ref=num_all.at[head_block, my_f, my_s],
            send_sem=num_ssem.at[t],
            recv_sem=num_rsem.at[head_block],
            device_id={"seq": t},
            device_id_type=MESH,
        )

    def sib_copy(o, to_f, to_s, from_f, from_s):
        slot = num_all.at[o, from_f, from_s]
        return pltpu.make_async_remote_copy(
            src_ref=slot,
            dst_ref=slot,
            send_sem=sib_ssem.at[o, to_f, to_s],
            recv_sem=sib_rsem.at[o, from_f, from_s],
            device_id={"fsdp": to_f, "sub": to_s},
            device_id_type=MESH,
        )

    def siblings():
        for df in range(nf):
            for ds in range(ns):
                if df or ds:
                    yield lax.rem(my_f + df, nf), lax.rem(my_s + ds, ns)

    def attend():
        gather_heads()
        for d in range(1, n):
            t = lax.rem(me + d, n)
            num_send[t] = numerator(t)
            num_copy(t, me).start()
        num_all[me, my_f, my_s] = numerator(me)
        for f, s in siblings():
            sib_copy(me, f, s, my_f, my_s).start()

    def spread():
        for d in range(1, n):
            o = lax.rem(me + d, n)
            num_copy(o, o).wait_recv()
            for f, s in siblings():
                sib_copy(o, f, s, my_f, my_s).start()

    for r in range(2, n):
        o_stream.relay(r, {2: attend, 3: spread}.get(r))

    for d in range(n):
        o = lax.rem(me + d, n)
        for f, s in siblings():
            sib_copy(o, f, s, f, s).wait_recv()

    head_width = nf * channels

    def attend_block(o, carry):
        for s in range(ns):
            whole = jnp.concatenate([num_all[o, f, s] for f in range(nf)], 0).astype(F32)
            meansq = jnp.sum(whole * whole, axis=0, keepdims=True) / head_width
            scaled = (whole * lax.rsqrt(meansq + 1e-06)).T * head_gain_ref[...]
            attended[o, :, s * head_width : (s + 1) * head_width] = scaled.astype(BF16)
        return carry

    lax.fori_loop(0, n, attend_block, 0)

    columns = out_ref.shape[1]
    depth = ns * head_width

    total[...] = jnp.dot(
        attended[me], wo_ref[...].reshape(depth, columns), preferred_element_type=F32
    )

    def multiply(o):
        o_stream.arrive(o)
        total[...] += jnp.dot(
            attended[o], wobuf[o].reshape(depth, columns), preferred_element_type=F32
        )

    for r in range(1, n):
        both(r, multiply)
    out_ref[...] = total[...].astype(BF16)

    w_stream.finish()
    o_stream.finish()
    for d in range(n):
        o = lax.rem(me + d, n)
        for df in range(nf):
            if d or df:
                other = lax.rem(my_f + df, nf)
                source = qk_send.at[o] if d else qk_all.at[me, my_f]
                qk_copy(o, source, other, me, my_f).wait_send()
        if d:
            v_copy(o, me).wait_send()
            num_copy(o, me).wait_send()
        for f, s in siblings():
            sib_copy(o, f, s, my_f, my_s).wait_send()

def line_kernel(
    n,
    pieces,
    early,
    row_chunks,
    tok_hbm,
    gain_ref,
    head_gain_ref,
    wo_hbm,
    wq_hbm,
    wk_hbm,
    wv_hbm,
    out_ref,
    tok_ref,
    wo_ref,
    load_sem,
    ysend,
    xn,
    xq,
    wall,
    wobuf,
    acc,
    part_send,
    part_recv,
    qk,
    q_full,
    kv,
    kv_prev,
    nacc,
    num_send,
    num_all,
    attended,
    total,
    w_ss,
    w_rs,
    tok_s,
    tok_r,
    o_out,
    o_in,
    o_rs,
    o_ac,
    o_yr,
    part_s,
    part_r,
    qk_s,
    qk_r,
    kv_s,
    kv_r,
    num_s,
    ng_s,
    ng_r,
):
    g = lax.axis_index("groups")
    z = lax.axis_index("seq")
    f = lax.axis_index("fsdp")
    s = lax.axis_index("sub")
    upper = z // (n // 2)
    sign = 2 * upper - 1
    out_z = z + sign
    in_z = z - sign
    inner = (z > 0) & (z < n - 1)
    outer = jnp.logical_not(inner)
    low = upper == 0
    high = upper == 1
    near = upper
    second = 1 - upper
    ends = n - 2
    my = jnp.where(inner, upper, ends + upper)
    sl_out = ends + upper
    sl_far = ends + 1 - upper
    p_own = 1 - upper
    p_end = upper
    tokens, width = tok_ref.shape
    rows, span = wall.shape[2], wall.shape[3]
    qk_rows = qk.shape[3]
    half_rows = qk_rows // 2
    quarter = f * 2 + s
    q_sib = f * 2 + 1 - s
    q_x = (1 - f) * 2 + s
    q_diag = (1 - f) * 2 + 1 - s

    loads = []
    for c in range(pieces):
        row = 0
        for source in (wq_hbm, wk_hbm, wv_hbm):
            size = source.shape[0]
            col = pl.multiple_of((g * pieces + c) * span, span)
            loads.append(
                pltpu.make_async_copy(
                    source.at[:, pl.ds(col, span)],
                    wall.at[c, my, pl.ds(row, size)],
                    load_sem.at[len(loads)],
                )
            )
            row += size
    wo_load = pltpu.make_async_copy(wo_hbm, wo_ref, load_sem.at[len(loads)])
    tok_load = pltpu.make_async_copy(tok_hbm, tok_ref, load_sem.at[len(loads) + 1])
    for load in loads + [wo_load, tok_load]:
        load.start()

    barrier = pltpu.get_barrier_semaphore()
    for peer in ({"seq": in_z}, {"groups": 1 - g}, {"fsdp": 1 - f}, {"sub": 1 - s}):
        pl.semaphore_signal(barrier, inc=1, device_id=peer, device_id_type=MESH)

    @pl.when(inner)
    def _():
        pl.semaphore_signal(barrier, inc=1, device_id={"seq": out_z}, device_id_type=MESH)
        pl.semaphore_wait(barrier, 5)

    @pl.when(outer)
    def _():
        pl.semaphore_wait(barrier, 4)

    logs = {"inner": [], "outer": [], "all": [], "low": []}

    def launch(role, make, *args):
        make(*args).start()
        logs[role].append((make, args))

    def remote(src, dst, send, recv, to):
        return pltpu.make_async_remote_copy(
            src_ref=src,
            dst_ref=dst,
            send_sem=send,
            recv_sem=recv,
            device_id=to,
            device_id_type=MESH,
        )

    def w_copy(h, c):
        slot = wall.at[c, h]
        return remote(slot, slot, w_ss.at[h, c], w_rs.at[h, c], {"seq": in_z})

    def o_copy(h, c, own, inward):
        slot = wobuf.at[h, g, c]
        return remote(
            wo_ref.at[g, c] if own else slot,
            slot,
            (o_in if inward else o_out).at[h, c],
            o_rs.at[h, c],
            {"seq": in_z if inward else out_z},
        )

    def across(h, c):
        slot = wobuf.at[h, g, c]
        return remote(slot, slot, o_ac.at[h, c], o_yr.at[h, c], {"groups": 1 - g})

    def crossed(h, c):
        slot = wobuf.at[h, 1 - g, c]
        remote(slot, slot, o_ac.at[h, c], o_yr.at[h, c], {"groups": 1 - g}).wait_recv()

    step = tokens // row_chunks

    def part_rows(r):
        return pl.ds(r * step, step)

    def y_tok(r):
        return remote(
            ysend.at[part_rows(r)],
            xq.at[0, quarter, part_rows(r)],
            tok_s.at[0, 0, r],
            tok_r.at[0, quarter, r],
            {"groups": 1 - g},
        )

    def z_tok(k, r):
        src = xn.at[quarter, part_rows(r)] if k == 1 else xq.at[0, quarter, part_rows(r)]
        return remote(
            src,
            xq.at[k, quarter, part_rows(r)],
            tok_s.at[k, 0, r],
            tok_r.at[k, quarter, r],
            {"seq": in_z},
        )

    def spread_tok(k, c, r, kind):
        slot = xq.at[k, c, part_rows(r)]
        to = {"fsdp": 1 - f} if kind == 2 else {"sub": 1 - s}
        return remote(slot, slot, tok_s.at[k, kind, r], tok_r.at[k, c, r], to)

    def tok_arrive(k, c, r):
        slot = xq.at[k, c, part_rows(r)]
        remote(slot, slot, tok_s.at[k, 1, r], tok_r.at[k, c, r], {"sub": 1 - s}).wait_recv()

    def gather_own(k, r):
        tok_arrive(k, quarter, r)
        launch("inner", spread_tok, k, quarter, r, 2)
        launch("inner", spread_tok, k, quarter, r, 1)

    def gather_fwd(k, r):
        tok_arrive(k, q_x, r)
        launch("inner", spread_tok, k, q_x, r, 3)

    def gathered(k, which):
        for r in range(row_chunks):
            for c in which:
                tok_arrive(k, c, r)

    def part_copy(p, h):
        return remote(
            part_send.at[p, h],
            part_recv.at[p, h],
            part_s.at[p, h],
            part_r.at[p, h],
            {"groups": 1 - g},
        )

    def qk_copy(p, h):
        slot = qk.at[p, h, f]
        return remote(slot, slot, qk_s.at[p, h], qk_r.at[p, h], {"fsdp": 1 - f})

    def qk_arrive(p, h):
        slot = qk.at[p, h, 1 - f]
        remote(slot, slot, qk_s.at[p, h], qk_r.at[p, h], {"fsdp": 1 - f}).wait_recv()

    def kv_copy(p, h):
        return remote(
            kv.at[p, h], kv_prev.at[p, h], kv_s.at[p, h], kv_r.at[p, h], {"seq": in_z}
        )

    def num_copy(h):
        return remote(
            num_send.at[h], num_all.at[h, f, s], num_s.at[h], ng_r.at[h, f, s], {"seq": out_z}
        )

    def spread_num(h, ff, ss, kind):
        slot = num_all.at[h, ff, ss]
        to = {"fsdp": 1 - f} if kind == 1 else {"sub": 1 - s}
        return remote(slot, slot, ng_s.at[h, kind], ng_r.at[h, ff, ss], to)

    def num_arrive(h, ff, ss):
        slot = num_all.at[h, ff, ss]
        remote(slot, slot, ng_s.at[h, 0], ng_r.at[h, ff, ss], {"sub": 1 - s}).wait_recv()

    @pl.when(inner)
    def _():
        for c in range(pieces):
            for load in loads[3 * c : 3 * c + 3]:
                load.wait()
            launch("inner", w_copy, my, c)
        wo_load.wait()
        for c in range(pieces):
            launch("inner", o_copy, my, c, True, False)

    @pl.when(outer)
    def _():
        for load in loads:
            load.wait()
        wo_load.wait()
        for c in range(early):
            launch("outer", o_copy, my, c, True, True)

    tok_load.wait()
    row_step = 16

    def norm_rows(i, carry):
        block = pl.ds(pl.multiple_of(i * row_step, row_step), row_step)
        sumsq = jnp.zeros((row_step, 1), F32)
        for c in range(2 * pieces):
            part = tok_ref[block, c * span : (c + 1) * span].astype(F32)
            sumsq = sumsq + jnp.sum(part * part, axis=1, keepdims=True)
        scale = lax.rsqrt(sumsq / width + 1e-05)

        def column(c):
            cols = pl.ds(pl.multiple_of(c * span, span), span)
            part = tok_ref[block, cols].astype(F32)
            return (part * scale * gain_ref[:, cols]).astype(BF16)

        ysend[block, :] = column((1 - g) * pieces + quarter)
        for c in range(pieces):
            xn[c, block, :] = column(g * pieces + c)
        return carry

    per_chunk = step // row_step
    for r in range(row_chunks):
        lax.fori_loop(r * per_chunk, (r + 1) * per_chunk, norm_rows, 0)
        launch("all", y_tok, r)

        @pl.when(outer)
        def _():
            launch("outer", z_tok, 1, r)

    def contract(weights, acts):
        return lax.dot_general(weights, acts, (((1,), (1,)), ((), ())), preferred_element_type=F32)

    def project(k, stack, lo, hi, fresh):
        if fresh:
            acc[k, stack] = jnp.zeros(acc.shape[2:], F32)

        def body(c, carry):
            weights = wall[c, 2 * stack : 2 * stack + 2].reshape(2 * rows, span)
            acts = xn[c] if k == 3 else xq[k, c]
            acc[k, stack] += contract(weights, acts)
            return carry

        lax.fori_loop(lo, hi, body, 0)

    def send_part(k, stack):
        p = p_own if k == 0 else p_end
        for i in range(2):
            h = 2 * stack + i
            part_send[p, h] = acc[k, stack, i * rows : (i + 1) * rows].astype(BF16)
            launch("inner", part_copy, p, h)

    def finish_proj(h, own):
        p, k = (p_own, 3) if own else (p_end, 1)
        part_copy(p, h).wait_recv()
        i = h % 2
        whole = acc[k, h // 2, i * rows : (i + 1) * rows] + part_recv[p, h].astype(F32)
        qk[p, h, f] = whole[:qk_rows].astype(BF16)
        kv[p, h, qk_rows:] = whole[qk_rows:].astype(BF16)
        launch("inner", qk_copy, p, h)

    def finish_qk(h, own):
        p = p_own if own else p_end
        qk_arrive(p, h)
        halves = [qk[p, h, i].astype(F32) for i in range(2)]
        q_full[p, h] = jnp.concatenate([x[:half_rows] for x in halves], 0).astype(BF16)
        kv[p, h, :qk_rows] = jnp.concatenate([x[half_rows:] for x in halves], 0).astype(BF16)

        @pl.when(low)
        def _():
            launch("low", kv_copy, p, h)

    key_pos = lax.broadcasted_iota(jnp.int32, (tokens, tokens), 0)
    query_pos = lax.broadcasted_iota(jnp.int32, (tokens, tokens), 1)

    def attend_to(source, queries, diagonal):
        scores = lax.dot_general(
            source[:qk_rows], queries, (((0,), (0,)), ((), ())), preferred_element_type=F32
        )
        value = 1.0 + scores * 0.25 + scores * scores * 0.03125
        if diagonal:
            value = jnp.where(key_pos <= query_pos, value, 0.0)
        return jnp.dot(source[qk_rows:], value.astype(BF16), preferred_element_type=F32)

    def prior_arrive(h):
        for p in range(2):
            kv_copy(p, h).wait_recv()

    def numerator(h, own):
        p = p_own if own else p_end
        queries = q_full[p, h]
        nacc[...] = attend_to(kv[p, h], queries, True)

        @pl.when(low if own else high)
        def _():
            nacc[...] += attend_to(kv[1 - p, h], queries, False)

        @pl.when(high)
        def _():
            nacc[...] += attend_to(kv_prev[0, h], queries, False) + attend_to(
                kv_prev[1, h], queries, False
            )

        if own:
            num_all[h, f, s] = nacc[...].astype(BF16)
            launch("inner", spread_num, h, f, s, 1)
            launch("inner", spread_num, h, f, s, 0)
        else:
            num_send[h] = nacc[...].astype(BF16)
            launch("inner", num_copy, h)

    def o_relay(role, h, c, inward):
        o_copy(h, c, False, True).wait_recv()
        if inward is not None:
            launch(role, o_copy, h, c, False, inward)
        launch(role, across, h, c)

    def w_relay(c):
        w_copy(sl_out, c).wait_recv()
        launch("inner", w_copy, sl_out, c)

    late = range(early, pieces)

    @pl.when(inner)
    def _():
        for c in range(pieces):
            launch("inner", o_copy, my, c, True, True)
        for c in range(early):
            o_relay("inner", sl_out, c, True)
        gather_own(0, 0)
        gather_own(1, 0)
        gather_own(0, 1)
        for c in range(pieces):
            w_copy(second, c).wait_recv()
        project(3, 0, 0, pieces, True)
        gather_fwd(0, 0)
        gather_own(1, 1)
        for c in range(2):
            o_relay("inner", second, c, False)
        gather_fwd(1, 0)
        gather_own(2, 0)
        for c in range(2, pieces):
            o_relay("inner", second, c, False)
        gather_fwd(0, 1)
        gathered(0, (q_sib, q_diag))
        project(0, 0, 0, pieces, True)
        send_part(0, 0)
        gather_own(2, 1)
        for c in range(early):
            o_relay("inner", sl_far, c, False)
        w_relay(0)
        gather_fwd(1, 1)
        gathered(1, (q_sib, q_diag))
        project(1, 0, 0, pieces, True)
        w_relay(1)
        for h in range(2):
            finish_proj(h, True)
        gather_fwd(2, 0)
        w_relay(2)
        w_relay(3)
        for h in range(2):
            finish_qk(h, True)
        gather_fwd(2, 1)
        gathered(2, (q_sib, q_diag))
        project(2, 0, 0, pieces, True)
        send_part(2, 0)
        for c in range(pieces - 1):
            w_copy(sl_far, c).wait_recv()
        for k in range(4):
            project(k, 1, 0, pieces - 1, True)
        for c in late:
            o_relay("inner", sl_out, c, True)
        for h in range(2):
            finish_proj(h, False)
        w_copy(sl_far, pieces - 1).wait_recv()
        for k in (2, 0):
            project(k, 1, pieces - 1, pieces, False)
            send_part(k, 1)
        for k in (3, 1):
            project(k, 1, pieces - 1, pieces, False)
        for h in range(2):
            finish_qk(h, False)

        def attention(h):
            @pl.when(high)
            def _():
                prior_arrive(h)

            numerator(h, False)
            numerator(h, True)

        for h in range(2):
            attention(h)
        for c in late:
            o_relay("inner", sl_far, c, False)
        for h in range(2, 4):
            finish_proj(h, False)
            finish_proj(h, True)
        for h in range(2, 4):
            finish_qk(h, False)
            finish_qk(h, True)
        for h in range(2, 4):
            attention(h)

    @pl.when(outer)
    def _():
        for r in range(row_chunks):
            tok_arrive(0, quarter, r)
            launch("outer", z_tok, 2, r)
        for c in range(pieces):
            launch("outer", w_copy, my, c)
        for c in late:
            launch("outer", o_copy, my, c, True, True)
        for h in (near, second):
            for c in range(pieces):
                o_relay("outer", h, c, None)
        for c in range(pieces):
            o_relay("outer", sl_far, c, None)
        for h in range(n):
            num_arrive(h, f, s)
            launch("outer", spread_num, h, f, s, 1)
            launch("outer", spread_num, h, f, s, 0)

    head_width = 2 * num_all.shape[3]
    columns = out_ref.shape[1]
    depth = 2 * head_width

    def attend_block(h):
        num_arrive(h, 1 - f, s)
        launch("all", spread_num, h, 1 - f, s, 2)
        num_arrive(h, f, 1 - s)
        num_arrive(h, 1 - f, 1 - s)
        for i in range(2):
            whole = jnp.concatenate([num_all[h, j, i] for j in range(2)], 0).astype(F32)
            meansq = jnp.sum(whole * whole, axis=0, keepdims=True) / head_width
            scaled = (whole * lax.rsqrt(meansq + 1e-06)).T * head_gain_ref[...]
            attended[h, :, i * head_width : (i + 1) * head_width] = scaled.astype(BF16)

    def multiply(h):
        @pl.when(my == h)
        def _():
            total[...] += jnp.dot(
                attended[h], wo_ref[...].reshape(depth, columns), preferred_element_type=F32
            )

        @pl.when(my != h)
        def _():
            for c in range(pieces):
                crossed(h, c)
            total[...] += jnp.dot(
                attended[h], wobuf[h].reshape(depth, columns), preferred_element_type=F32
            )

    total[...] = jnp.zeros(total.shape, F32)
    for h in range(n):
        attend_block(h)
        multiply(h)
    out_ref[...] = total[...].astype(BF16)

    for role, gate in (("inner", inner), ("outer", outer), ("low", inner & low)):

        @pl.when(gate)
        def _():
            for make, args in logs[role]:
                make(*args).wait_send()

    for make, args in logs["all"]:
        make(*args).wait_send()


def per_device_line(n, tokens, norm_gain, w_query, w_key, w_value, head_gain, w_out):
    count, width = tokens.shape
    shards = [w_query[0], w_key[0], w_value[0]]
    rows = sum(shard.shape[0] for shard in shards)
    qk_rows = w_query.shape[1] + w_key.shape[1]
    channels = w_value.shape[1]
    head_width, columns = w_out.shape[1], w_out.shape[2]
    pieces, early, row_chunks = 4, 2, 2
    span = width // (2 * pieces)
    wo = w_out.reshape(2, pieces, head_width // pieces, columns)
    hbm = pl.BlockSpec(memory_space=pl.ANY)
    vmem = pl.BlockSpec(memory_space=pltpu.VMEM)
    dma = pltpu.SemaphoreType.DMA
    return pl.pallas_call(
        functools.partial(line_kernel, n, pieces, early, row_chunks),
        out_shape=jax.ShapeDtypeStruct((count, columns), BF16),
        in_specs=[hbm, vmem, vmem, hbm] + [hbm] * 3,
        out_specs=vmem,
        scratch_shapes=[
            pltpu.VMEM(tokens.shape, BF16),
            pltpu.VMEM(wo.shape, BF16),
            dma((3 * pieces + 2,)),
            pltpu.VMEM((count, span), BF16),
            pltpu.VMEM((pieces, count, span), BF16),
            pltpu.VMEM((3, pieces, count, span), BF16),
            pltpu.VMEM((pieces, n, rows, span), BF16),
            pltpu.VMEM((n,) + wo.shape, BF16),
            pltpu.VMEM((4, n // 2, 2 * rows, count), F32),
            pltpu.VMEM((2, n, rows, count), BF16),
            pltpu.VMEM((2, n, rows, count), BF16),
            pltpu.VMEM((2, n, 2, qk_rows, count), BF16),
            pltpu.VMEM((2, n, qk_rows, count), BF16),
            pltpu.VMEM((2, n, rows, count), BF16),
            pltpu.VMEM((2, n, rows, count), BF16),
            pltpu.VMEM((channels, count), F32),
            pltpu.VMEM((n, channels, count), BF16),
            pltpu.VMEM((n, 2, 2, channels, count), BF16),
            pltpu.VMEM((n, count, 2 * head_width), BF16),
            pltpu.VMEM((count, columns), F32),
            dma((n, pieces)),
            dma((n, pieces)),
            dma((3, 4, row_chunks)),
            dma((3, pieces, row_chunks)),
            dma((n, pieces)),
            dma((n, pieces)),
            dma((n, pieces)),
            dma((n, pieces)),
            dma((n, pieces)),
            dma((2, n)),
            dma((2, n)),
            dma((2, n)),
            dma((2, n)),
            dma((2, n)),
            dma((2, n)),
            dma((n,)),
            dma((n, 3)),
            dma((n, 2, 2)),
        ],
        compiler_params=pltpu.CompilerParams(
            collective_id=0, has_side_effects=True, vmem_limit_bytes=60 * 1024 * 1024
        ),
    )(tokens, norm_gain.reshape(1, -1), head_gain.reshape(1, -1), wo, *shards)


def per_device(sizes, tokens, norm_gain, w_query, w_key, w_value, head_gain, w_out):
    n, nf, ns = sizes
    shards = [w_query[0], w_key[0], w_value[0]]
    if any(shard.shape[0] % 8 for shard in shards):
        shards = [jnp.concatenate(shards, 0)]
    rows, width = sum(shard.shape[0] for shard in shards), tokens.shape[1]
    count = tokens.shape[0]
    qk_rows = w_query.shape[1] + w_key.shape[1]
    channels = w_value.shape[1]
    head_width, columns = w_out.shape[1], w_out.shape[2]
    pieces = max(1, 16 // n)
    out_pieces = max(1, 16 // n)
    wo = w_out.reshape(ns, out_pieces, head_width // out_pieces, columns)
    hbm = pl.BlockSpec(memory_space=pl.ANY)
    vmem = pl.BlockSpec(memory_space=pltpu.VMEM)
    dma = pltpu.SemaphoreType.DMA
    return pl.pallas_call(
        functools.partial(kernel, n, nf, ns, pieces, out_pieces, len(shards)),
        out_shape=jax.ShapeDtypeStruct((count, columns), BF16),
        in_specs=[hbm, vmem, vmem, hbm] + [hbm] * len(shards),
        out_specs=vmem,
        scratch_shapes=[
            pltpu.VMEM(tokens.shape, BF16),
            pltpu.VMEM((rows, width), BF16),
            pltpu.VMEM(wo.shape, BF16),
            dma((len(shards) + 2,)),
            pltpu.VMEM((2 * pieces, count, width // (2 * pieces)), BF16),
            pltpu.VMEM((n, 2, pieces, rows, width // (2 * pieces)), BF16),
            pltpu.VMEM((n,) + wo.shape, BF16),
            pltpu.VMEM((n, qk_rows, count), BF16),
            pltpu.VMEM((n, channels, count), BF16),
            pltpu.VMEM((n, nf, qk_rows, count), BF16),
            pltpu.VMEM((n, channels, count), BF16),
            pltpu.VMEM((n, nf * qk_rows // 2, count), BF16),
            pltpu.VMEM((n, nf * qk_rows // 2, count), BF16),
            pltpu.VMEM((n, channels, count), BF16),
            pltpu.VMEM((n, nf, ns, channels, count), BF16),
            pltpu.VMEM((n, count, ns * head_width), BF16),
            pltpu.VMEM((count, columns), F32),
        ]
        + [dma((n, pieces))] * 5
        + [dma((n, out_pieces))] * 5
        + [
            dma((n, nf)),
            dma((n, nf)),
            dma((n,)),
            dma((n,)),
            dma((n,)),
            dma((n,)),
            dma((n, nf, ns)),
            dma((n, nf, ns)),
        ],
        compiler_params=pltpu.CompilerParams(
            collective_id=0, has_side_effects=True, vmem_limit_bytes=60 * 1024 * 1024
        ),
    )(tokens, norm_gain.reshape(1, -1), head_gain.reshape(1, -1), wo, *shards)


def solution(mesh):
    in_specs = (
        P(("groups", "seq"), None),
        P(),
        P(("seq", "sub"), "fsdp", None),
        P(("seq", "sub"), "fsdp", None),
        P(("seq", "sub"), "fsdp", None),
        P(),
        P("seq", None, ("fsdp", "sub")),
    )
    out_specs = P(("groups", "seq"), ("fsdp", "sub"))
    sizes = (mesh.shape["seq"], mesh.shape["fsdp"], mesh.shape["sub"])
    if sizes == (4, 2, 2):
        body = functools.partial(per_device_line, sizes[0])
    else:
        body = functools.partial(per_device, sizes)
    return jax.shard_map(
        body,
        mesh=mesh,
        in_specs=in_specs,
        out_specs=out_specs,
        check_vma=False,
    )
```

```python
import functools

import jax
import jax.numpy as jnp
from jax import lax
from jax.experimental import pallas as pl
from jax.experimental.pallas import tpu as pltpu
from jax.sharding import PartitionSpec as P

MESH = pl.DeviceIdType.MESH
F32 = jnp.float32
BF16 = jnp.bfloat16


def kernel(
    n,
    nf,
    ns,
    pieces,
    out_pieces,
    w_count,
    tok_hbm,
    gain_ref,
    head_gain_ref,
    wo_hbm,
    *rest,
):
    kernel_body(
        n, nf, ns, pieces, out_pieces, tok_hbm, gain_ref, head_gain_ref, wo_hbm,
        rest[:w_count], *rest[w_count:]
    )


def kernel_body(
    n,
    nf,
    ns,
    pieces,
    out_pieces,
    tok_hbm,
    gain_ref,
    head_gain_ref,
    wo_hbm,
    w_hbm,
    out_ref,
    tok_ref,
    w_ref,
    wo_ref,
    load_sem,
    normed,
    wbuf,
    wobuf,
    qk_send,
    v_send,
    qk_all,
    v_all,
    q_full,
    k_full,
    num_send,
    num_all,
    attended,
    total,
    w_zrecv,
    w_yrecv,
    w_right,
    w_left,
    w_across,
    o_zrecv,
    o_yrecv,
    o_right,
    o_left,
    o_across,
    qk_ssem,
    qk_rsem,
    v_ssem,
    v_rsem,
    num_ssem,
    num_rsem,
    sib_ssem,
    sib_rsem,
):
    group = lax.axis_index("groups")
    me = lax.axis_index("seq")
    my_f = lax.axis_index("fsdp")
    my_s = lax.axis_index("sub")
    tokens, width = tok_ref.shape

    loads = []
    row = 0
    for k, source in enumerate(w_hbm):
        size = source.shape[0]
        target = w_ref.at[pl.ds(row, size)] if len(w_hbm) > 1 else w_ref
        loads.append(pltpu.make_async_copy(source, target, load_sem.at[k]))
        row += size
    tok_load = pltpu.make_async_copy(tok_hbm, tok_ref, load_sem.at[len(w_hbm)])
    wo_load = pltpu.make_async_copy(wo_hbm, wo_ref, load_sem.at[len(w_hbm) + 1])
    for load in loads + [tok_load, wo_load]:
        load.start()

    peers = [
        {"seq": lax.rem(me + dz, n), "fsdp": lax.rem(my_f + df, nf)}
        for dz in range(n)
        for df in range(nf)
        if dz or df
    ]
    peers += [
        {"fsdp": lax.rem(my_f + df, nf), "sub": lax.rem(my_s + ds, ns)}
        for df in range(nf)
        for ds in range(1, ns)
    ]
    peers += [{"groups": 1 - group}]
    barrier = pltpu.get_barrier_semaphore()
    for peer in peers:
        pl.semaphore_signal(barrier, inc=1, device_id=peer, device_id_type=MESH)
    pl.semaphore_wait(barrier, len(peers))
    for load in loads:
        load.wait()
    span = width // (2 * pieces)
    qk_rows = qk_all.shape[2]
    half_rows = qk_rows // 2

    def own_w(c):
        start = pl.multiple_of((group * pieces + c) * span, span)
        return w_ref.at[:, pl.ds(start, span)]

    def own_o(c):
        return wo_ref.at[group, c]

    class Stream:
        def __init__(self, own, buf, count, zrecv, yrecv, right, left, across):
            self.own, self.buf, self.count = own, buf, count
            self.zrecv, self.yrecv = zrecv, yrecv
            self.right_sem, self.left_sem, self.across_sem = right, left, across

        def along(self, o, c, sems, target, own):
            slot = self.buf.at[o, group, c]
            return pltpu.make_async_remote_copy(
                src_ref=self.own(c) if own else slot,
                dst_ref=slot,
                send_sem=sems.at[o, c],
                recv_sem=self.zrecv.at[o, c],
                device_id={"seq": target},
                device_id_type=MESH,
            )

        def right(self, o, c, own=False):
            return self.along(o, c, self.right_sem, me + 1, own)

        def left(self, o, c, own=False):
            return self.along(o, c, self.left_sem, me - 1, own)

        def across(self, o, c, half):
            slot = self.buf.at[o, half, c]
            return pltpu.make_async_remote_copy(
                src_ref=slot,
                dst_ref=slot,
                send_sem=self.across_sem.at[o, c],
                recv_sem=self.yrecv.at[o, c],
                device_id={"groups": 1 - group},
                device_id_type=MESH,
            )

        def begin(self):
            for c in range(self.count):

                @pl.when(me + 1 < n)
                def _():
                    self.right(me, c, True).start()

                @pl.when(me >= 1)
                def _():
                    self.left(me, c, True).start()

        def relay(self, r, between=None):
            for c in range(self.count):
                if between is not None and c == self.count // 2:
                    between()

                @pl.when(me >= r)
                def _():
                    o = me - r
                    self.right(o, c).wait_recv()

                    @pl.when(me + 1 < n)
                    def _():
                        self.right(o, c).start()

                    self.across(o, c, group).start()

                @pl.when(me + r < n)
                def _():
                    o = me + r
                    self.left(o, c).wait_recv()

                    @pl.when(me >= 1)
                    def _():
                        self.left(o, c).start()

                    self.across(o, c, group).start()

        def arrive(self, o):
            for c in range(self.count):
                self.across(o, c, 1 - group).wait_recv()

        def finish(self):
            for r in range(n):
                for c in range(self.count):

                    @pl.when((me >= r) & (me + 1 < n))
                    def _():
                        self.right(me - r, c, r == 0).wait_send()

                    @pl.when((me + r < n) & (me >= 1))
                    def _():
                        self.left(me + r, c, r == 0).wait_send()

                    if r > 0:

                        @pl.when(me >= r)
                        def _():
                            self.across(me - r, c, group).wait_send()

                        @pl.when(me + r < n)
                        def _():
                            self.across(me + r, c, group).wait_send()

    w_stream = Stream(own_w, wbuf, pieces, w_zrecv, w_yrecv, w_right, w_left, w_across)
    o_stream = Stream(own_o, wobuf, out_pieces, o_zrecv, o_yrecv, o_right, o_left, o_across)

    w_stream.begin()
    wo_load.wait()
    at_end = (me == 0) | (me == n - 1)

    @pl.when(at_end)
    def _():
        o_stream.begin()

    tok_load.wait()

    row_step = 16

    def norm_rows(i, carry):
        rows = pl.ds(pl.multiple_of(i * row_step, row_step), row_step)
        sumsq = jnp.zeros((row_step, 1), F32)
        for c in range(2 * pieces):
            part = tok_ref[rows, c * span : (c + 1) * span].astype(F32)
            sumsq = sumsq + jnp.sum(part * part, axis=1, keepdims=True)
        scale = lax.rsqrt(sumsq / width + 1e-05)
        for c in range(2 * pieces):
            cols = slice(c * span, (c + 1) * span)
            part = tok_ref[rows, cols].astype(F32)
            normed[c, rows, :] = (part * scale * gain_ref[:, cols]).astype(BF16)
        return carry

    lax.fori_loop(0, tokens // row_step, norm_rows, 0)

    def contract(weights, acts):
        return lax.dot_general(weights, acts, (((1,), (1,)), ((), ())), preferred_element_type=F32)

    def qk_copy(o, source, other_f, token_block, f_from):
        return pltpu.make_async_remote_copy(
            src_ref=source,
            dst_ref=qk_all.at[token_block, f_from],
            send_sem=qk_ssem.at[o, other_f],
            recv_sem=qk_rsem.at[token_block, f_from],
            device_id={"seq": o, "fsdp": other_f},
            device_id_type=MESH,
        )

    def v_copy(o, token_block):
        return pltpu.make_async_remote_copy(
            src_ref=v_send.at[o],
            dst_ref=v_all.at[token_block],
            send_sem=v_ssem.at[o],
            recv_sem=v_rsem.at[token_block],
            device_id={"seq": o},
            device_id_type=MESH,
        )

    def project_own():
        acc = jnp.zeros((w_ref.shape[0], tokens), F32)
        for c in range(2 * pieces):
            acc = acc + contract(w_ref[:, c * span : (c + 1) * span], normed[c])
        qk_all[me, my_f] = acc[:qk_rows].astype(BF16)
        v_all[me] = acc[qk_rows:].astype(BF16)
        for df in range(1, nf):
            other = lax.rem(my_f + df, nf)
            qk_copy(me, qk_all.at[me, my_f], other, me, my_f).start()

    def project(o):
        def body(c, acc):
            return acc + contract(wbuf[o, c // pieces, c % pieces], normed[c])

        acc = lax.fori_loop(0, 2 * pieces, body, jnp.zeros((w_ref.shape[0], tokens), F32))
        qk_send[o] = acc[:qk_rows].astype(BF16)
        v_send[o] = acc[qk_rows:].astype(BF16)
        for df in range(nf):
            qk_copy(o, qk_send.at[o], lax.rem(my_f + df, nf), me, my_f).start()
        v_copy(o, me).start()

    def both(r, action):
        @pl.when(me >= r)
        def _():
            action(me - r)

        @pl.when(me + r < n)
        def _():
            action(me + r)

    def take(o):
        w_stream.arrive(o)
        project(o)

    project_own()
    for r in range(1, n):
        if r == n - 1:

            @pl.when(jnp.logical_not(at_end))
            def _():
                o_stream.begin()

        w_stream.relay(r, functools.partial(both, r - 1, take) if r > 1 else None)

    o_stream.relay(1, functools.partial(both, n - 1, take))

    def gather_heads():
        for d in range(1, n):
            t = lax.rem(me + d, n)
            v_copy(me, t).wait_recv()
            for df in range(nf):
                qk_copy(me, qk_all.at[t, df], 0, t, df).wait_recv()
        for df in range(1, nf):
            other = lax.rem(my_f + df, nf)
            qk_copy(me, qk_all.at[me, other], other, me, other).wait_recv()

        for t in range(n):
            parts = [qk_all[t, f].astype(F32) for f in range(nf)]
            q_full[t] = jnp.concatenate([p[:half_rows] for p in parts], 0).astype(BF16)
            k_full[t] = jnp.concatenate([p[half_rows:] for p in parts], 0).astype(BF16)

    channels = v_all.shape[1]
    key_pos = lax.broadcasted_iota(jnp.int32, (tokens, tokens), 0)
    query_pos = lax.broadcasted_iota(jnp.int32, (tokens, tokens), 1)

    def numerator(t):
        queries = q_full[t]

        def body(j, acc):
            scores = lax.dot_general(
                k_full[j], queries, (((0,), (0,)), ((), ())), preferred_element_type=F32
            )
            value = 1.0 + scores * 0.25 + scores * scores * 0.03125
            weight = jnp.where(key_pos + (j - t) * tokens <= query_pos, value, 0.0).astype(BF16)
            return acc + jnp.dot(v_all[j], weight, preferred_element_type=F32)

        acc = lax.fori_loop(0, t + 1, body, jnp.zeros((channels, tokens), F32))
        return acc.astype(BF16)

    def num_copy(t, head_block):
        return pltpu.make_async_remote_copy(
            src_ref=num_send.at[t],
            dst_ref=num_all.at[head_block, my_f, my_s],
            send_sem=num_ssem.at[t],
            recv_sem=num_rsem.at[head_block],
            device_id={"seq": t},
            device_id_type=MESH,
        )

    def sib_copy(o, to_f, to_s, from_f, from_s):
        slot = num_all.at[o, from_f, from_s]
        return pltpu.make_async_remote_copy(
            src_ref=slot,
            dst_ref=slot,
            send_sem=sib_ssem.at[o, to_f, to_s],
            recv_sem=sib_rsem.at[o, from_f, from_s],
            device_id={"fsdp": to_f, "sub": to_s},
            device_id_type=MESH,
        )

    def siblings():
        for df in range(nf):
            for ds in range(ns):
                if df or ds:
                    yield lax.rem(my_f + df, nf), lax.rem(my_s + ds, ns)

    def attend():
        gather_heads()
        for d in range(1, n):
            t = lax.rem(me + d, n)
            num_send[t] = numerator(t)
            num_copy(t, me).start()
        num_all[me, my_f, my_s] = numerator(me)
        for f, s in siblings():
            sib_copy(me, f, s, my_f, my_s).start()

    def spread():
        for d in range(1, n):
            o = lax.rem(me + d, n)
            num_copy(o, o).wait_recv()
            for f, s in siblings():
                sib_copy(o, f, s, my_f, my_s).start()

    for r in range(2, n):
        o_stream.relay(r, {2: attend, 3: spread}.get(r))

    for d in range(n):
        o = lax.rem(me + d, n)
        for f, s in siblings():
            sib_copy(o, f, s, f, s).wait_recv()

    head_width = nf * channels

    def attend_block(o, carry):
        for s in range(ns):
            whole = jnp.concatenate([num_all[o, f, s] for f in range(nf)], 0).astype(F32)
            meansq = jnp.sum(whole * whole, axis=0, keepdims=True) / head_width
            scaled = (whole * lax.rsqrt(meansq + 1e-06)).T * head_gain_ref[...]
            attended[o, :, s * head_width : (s + 1) * head_width] = scaled.astype(BF16)
        return carry

    lax.fori_loop(0, n, attend_block, 0)

    columns = out_ref.shape[1]
    depth = ns * head_width

    total[...] = jnp.dot(
        attended[me], wo_ref[...].reshape(depth, columns), preferred_element_type=F32
    )

    def multiply(o):
        o_stream.arrive(o)
        total[...] += jnp.dot(
            attended[o], wobuf[o].reshape(depth, columns), preferred_element_type=F32
        )

    for r in range(1, n):
        both(r, multiply)
    out_ref[...] = total[...].astype(BF16)

    w_stream.finish()
    o_stream.finish()
    for d in range(n):
        o = lax.rem(me + d, n)
        for df in range(nf):
            if d or df:
                other = lax.rem(my_f + df, nf)
                source = qk_send.at[o] if d else qk_all.at[me, my_f]
                qk_copy(o, source, other, me, my_f).wait_send()
        if d:
            v_copy(o, me).wait_send()
            num_copy(o, me).wait_send()
        for f, s in siblings():
            sib_copy(o, f, s, my_f, my_s).wait_send()

def line_kernel(
    n,
    pieces,
    w_pieces,
    out_pieces,
    early,
    whole_pieces,
    direct,
    row_chunks,
    tok_hbm,
    gain_ref,
    head_gain_ref,
    wo_hbm,
    wq_hbm,
    wk_hbm,
    wv_hbm,
    out_hbm,
    tok_ref,
    wo_ref,
    out_ref,
    load_sem,
    out_sem,
    ysend,
    ysend2,
    xn,
    xq,
    wall,
    wobuf,
    acc,
    part_send,
    part_recv,
    qk,
    q_full,
    kv,
    kv_prev,
    qk_mine,
    nacc,
    num_send,
    num_all,
    attended,
    total,
    w_ss,
    w_rs,
    tok_s,
    tok_r,
    o_out,
    o_in,
    o_rs,
    o_ac,
    o_yr,
    part_s,
    part_r,
    qk_s,
    qk_r,
    kv_s,
    kv_r,
    num_s,
    ng_s,
    ng_r,
    beyond,
):
    g = lax.axis_index("groups")
    z = lax.axis_index("seq")
    f = lax.axis_index("fsdp")
    s = lax.axis_index("sub")
    upper = z // (n // 2)
    sign = 2 * upper - 1
    out_z = z + sign
    in_z = z - sign
    inner = (z > 0) & (z < n - 1)
    outer = jnp.logical_not(inner)
    low = upper == 0
    high = upper == 1
    near = upper
    second = 1 - upper
    ends = n - 2
    my = jnp.where(inner, upper, ends + upper)
    sl_out = ends + upper
    sl_far = ends + 1 - upper
    p_own = 1 - upper
    p_end = upper
    tokens, width = tok_ref.shape
    rows, w_span = wall.shape[2], wall.shape[3]
    span = xn.shape[2]
    split = span // w_span
    qk_rows = qk.shape[3]
    half_rows = qk_rows // 2
    quarter = f * 2 + s
    f_other = 1 - f
    q_sib = f * 2 + 1 - s
    q_x = (1 - f) * 2 + s
    q_diag = (1 - f) * 2 + 1 - s

    loads = []
    for c in range(w_pieces):
        row = 0
        for source in (wq_hbm, wk_hbm, wv_hbm):
            size = source.shape[0]
            col = pl.multiple_of((g * w_pieces + c) * w_span, w_span)
            loads.append(
                pltpu.make_async_copy(
                    source.at[:, pl.ds(col, w_span)],
                    wall.at[c, my, pl.ds(row, size)],
                    load_sem.at[c],
                )
            )
            row += size

    def w_loaded(c):
        slot = wall.at[c, my]
        pltpu.make_async_copy(slot, slot, load_sem.at[c]).wait()

    wo_load = pltpu.make_async_copy(wo_hbm, wo_ref, load_sem.at[w_pieces])
    step = tokens // row_chunks
    tok_loads = [
        pltpu.make_async_copy(
            tok_hbm.at[pl.ds(r * step, step)],
            tok_ref.at[pl.ds(r * step, step)],
            load_sem.at[w_pieces + 1 + r],
        )
        for r in range(row_chunks)
    ]
    for load in loads + [wo_load] + tok_loads:
        load.start()

    barrier = pltpu.get_barrier_semaphore()
    for peer in (
        {"seq": in_z},
        {"groups": 1 - g},
        {"fsdp": 1 - f},
        {"sub": 1 - s},
    ):
        pl.semaphore_signal(barrier, inc=1, device_id=peer, device_id_type=MESH)

    @pl.when(inner)
    def _():
        pl.semaphore_signal(barrier, inc=1, device_id={"seq": out_z}, device_id_type=MESH)
        pl.semaphore_wait(barrier, 5)
        pl.semaphore_signal(beyond, inc=1, device_id={"fsdp": 1 - f}, device_id_type=MESH)

    @pl.when(outer)
    def _():
        pl.semaphore_wait(barrier, 4)

    logs = {"inner": [], "outer": [], "all": [], "low": []}

    def launch(role, make, *args):
        make(*args).start()
        logs[role].append((make, args))

    def remote(src, dst, send, recv, to):
        return pltpu.make_async_remote_copy(
            src_ref=src,
            dst_ref=dst,
            send_sem=send,
            recv_sem=recv,
            device_id=to,
            device_id_type=MESH,
        )

    def w_copy(h, c):
        slot = wall.at[c, h]
        return remote(slot, slot, w_ss.at[h], w_rs.at[h, c], {"seq": in_z})

    def o_copy(h, c, own, inward):
        slot = wobuf.at[h, g, c]
        return remote(
            wo_ref.at[g, c] if own else slot,
            slot,
            (o_in if inward else o_out).at[h],
            o_rs.at[h, c],
            {"seq": in_z if inward else out_z},
        )

    def o_other(c):
        return remote(
            wo_ref.at[1 - g, c], wobuf.at[my, 1 - g, c], o_ac.at[my], o_yr.at[my], {"seq": in_z}
        )

    def across(h, c):
        slot = wobuf.at[h, g, c]
        return remote(slot, slot, o_ac.at[h], o_yr.at[h], {"groups": 1 - g})

    def crossed(h):
        slot = wobuf.at[h, 1 - g]
        remote(slot, slot, o_ac.at[h], o_yr.at[h], {"groups": 1 - g}).wait_recv()

    def part_rows(r):
        return pl.ds(r * step, step)

    def y_tok(r):
        return remote(
            ysend.at[part_rows(r)],
            xq.at[0, quarter, part_rows(r)],
            tok_s.at[0, 0],
            tok_r.at[0, quarter, r],
            {"groups": 1 - g},
        )

    def y_tok2(r):
        return remote(
            ysend2.at[part_rows(r)],
            xq.at[0, q_x, part_rows(r)],
            tok_s.at[0, 2],
            tok_r.at[0, q_x, r],
            {"groups": 1 - g},
        )

    def z_tok(k, r):
        src = xn.at[quarter, part_rows(r)] if k == 1 else xq.at[0, quarter, part_rows(r)]
        return remote(
            src,
            xq.at[k, quarter, part_rows(r)],
            tok_s.at[k, 0],
            tok_r.at[k, quarter, r],
            {"seq": in_z},
        )

    def spread_tok(k, c, r, kind):
        slot = xq.at[k, c, part_rows(r)]
        to = {"fsdp": 1 - f} if kind == 2 else {"sub": 1 - s}
        return remote(slot, slot, tok_s.at[k, kind], tok_r.at[k, c, r], to)

    def tok_arrive(k, c, r):
        slot = xq.at[k, c, part_rows(r)]
        remote(slot, slot, tok_s.at[k, 1], tok_r.at[k, c, r], {"sub": 1 - s}).wait_recv()

    def gather_own(k, r):
        tok_arrive(k, quarter, r)
        if k > 0 or r < direct:
            spread_tok(k, quarter, r, 2).start()
        spread_tok(k, quarter, r, 1).start()

    def gather_fwd(k, r):
        tok_arrive(k, q_x, r)
        spread_tok(k, q_x, r, 3).start()

    def gathered(k, which):
        for r in range(row_chunks):
            for c in which:
                tok_arrive(k, c, r)

    def both(stack):
        return pl.ds(2 * stack, 2)

    def part_copy(p, stack):
        return remote(
            part_send.at[p, both(stack)],
            part_recv.at[p, both(stack)],
            part_s.at[p, stack],
            part_r.at[p, stack],
            {"groups": 1 - g},
        )

    def qk_copy(p, stack, way):
        if way:
            src = part_send.at[p, both(stack), pl.ds(0, qk_rows)]
            to = {"groups": 1 - g, "fsdp": 1 - f}
        else:
            src, to = qk_mine.at[p, both(stack)], {"fsdp": 1 - f}
        return remote(
            src, qk.at[p, way, both(stack)], qk_s.at[p, stack, way], qk_r.at[p, stack, way], to
        )

    def lanes(p):
        start = p * tokens
        return pl.ds(start if isinstance(p, int) else pl.multiple_of(start, tokens), tokens)

    def kv_copy(p, stack):
        there = (both(stack), slice(None), lanes(p))
        return remote(
            kv.at[there], kv_prev.at[there], kv_s.at[p, stack], kv_r.at[p, stack], {"seq": in_z}
        )

    def num_copy(stack):
        return remote(
            num_send.at[both(stack)],
            num_all.at[both(stack), f, s],
            num_s.at[stack],
            ng_r.at[stack, f, s],
            {"seq": out_z},
        )

    def spread_num(stack, kind):
        ff = f_other if kind == 2 else f
        slot = num_all.at[both(stack), ff, s]
        to = {"fsdp": 1 - f} if kind == 1 else {"sub": 1 - s}
        return remote(slot, slot, ng_s.at[stack, kind], ng_r.at[stack, ff, s], to)

    def num_arrive(stack, ff, ss):
        slot = num_all.at[both(stack), ff, ss]
        remote(slot, slot, ng_s.at[stack, 0], ng_r.at[stack, ff, ss], {"sub": 1 - s}).wait_recv()

    def nums_taken(stack):
        num_arrive(stack, f, s)
        for kind in (1, 0):
            spread_num(stack, kind).start()

    def nums_passed(stack):
        num_arrive(stack, 1 - f, s)
        spread_num(stack, 2).start()

    def nums_gathered(stack):
        num_arrive(stack, f, 1 - s)
        num_arrive(stack, 1 - f, 1 - s)

    @pl.when(inner)
    def _():
        for c in range(w_pieces):
            w_loaded(c)
            w_copy(my, c).start()
        wo_load.wait()
        for c in range(out_pieces):
            o_copy(my, c, True, False).start()

    @pl.when(outer)
    def _():
        wo_load.wait()
        for c in range(early):
            o_copy(my, c, True, True).start()

    row_step = 16

    def norm_rows(i, carry):
        block = pl.ds(pl.multiple_of(i * row_step, row_step), row_step)
        sumsq = jnp.zeros((row_step, 1), F32)
        for c in range(2 * pieces):
            part = tok_ref[block, c * span : (c + 1) * span].astype(F32)
            sumsq = sumsq + jnp.sum(part * part, axis=1, keepdims=True)
        scale = lax.rsqrt(sumsq / width + 1e-05)

        def column(c):
            cols = pl.ds(pl.multiple_of(c * span, span), span)
            part = tok_ref[block, cols].astype(F32)
            return (part * scale * gain_ref[:, cols]).astype(BF16)

        ysend[block, :] = column((1 - g) * pieces + quarter)
        ysend2[block, :] = column((1 - g) * pieces + q_x)
        for c in range(pieces):
            xn[c, block, :] = column(g * pieces + c)
        return carry

    per_chunk = step // row_step
    for r in range(row_chunks):
        tok_loads[r].wait()
        lax.fori_loop(r * per_chunk, (r + 1) * per_chunk, norm_rows, 0)
        y_tok(r).start()

        @pl.when(outer)
        def _():
            z_tok(1, r).start()

    @pl.when(inner)
    def _():
        for r in range(direct, row_chunks):
            y_tok2(r).start()

    def contract(weights, acts):
        return lax.dot_general(weights, acts, (((1,), (1,)), ((), ())), preferred_element_type=F32)

    def project(k, stack, lo, hi, fresh):
        if fresh:
            acc[k, stack] = jnp.zeros(acc.shape[2:], F32)

        def dot(j, i):
            weights = wall[j * split + i, 2 * stack : 2 * stack + 2].reshape(2 * rows, w_span)
            where = pl.ds(i * w_span, w_span)
            return contract(weights, xn[j, :, where] if k == 3 else xq[k, j, :, where])

        def body(j, carry):
            acc[k, stack] += sum([dot(j, i) for i in range(1, split)], dot(j, 0))
            return carry

        lax.fori_loop(lo // split, hi // split, body, 0)

    def send_part(k, stack):
        p = p_own if k == 0 else p_end
        for i in range(2):
            part_send[p, 2 * stack + i] = acc[k, stack, i * rows : (i + 1) * rows].astype(BF16)
        launch("inner", qk_copy, p, stack, 1)
        launch("inner", part_copy, p, stack)

    def send_qk(k, stack):
        p = p_own if k == 3 else p_end
        for i in range(2):
            part = acc[k, stack, i * rows : i * rows + qk_rows]
            qk_mine[p, 2 * stack + i] = part.astype(BF16)
        launch("inner", qk_copy, p, stack, 0)

    def finish_proj(stack, own):
        p, k = (p_own, 3) if own else (p_end, 1)
        part_copy(p, stack).wait_recv()
        for way in range(2):
            qk_copy(p, stack, way).wait_recv()
        for i in range(2):
            h = 2 * stack + i
            whole = acc[k, stack, i * rows : (i + 1) * rows] + part_recv[p, h].astype(F32)
            mine = whole[:qk_rows].astype(BF16).astype(F32)
            other = qk[p, 0, h].astype(F32) + qk[p, 1, h].astype(F32)
            lower = jnp.where(f == 0, mine, other)
            higher = jnp.where(f == 0, other, mine)

            def dims(first):
                last = first + half_rows
                return jnp.concatenate([lower[first:last], higher[first:last]], 0).astype(BF16)

            q_full[h, pl.ds(0, qk_rows), lanes(p)] = dims(0)
            kv[h, pl.ds(0, qk_rows), lanes(p)] = dims(half_rows)
            kv[h, pl.ds(qk_rows, rows - qk_rows), lanes(p)] = whole[qk_rows:].astype(BF16)

        @pl.when(low)
        def _():
            launch("low", kv_copy, p, stack)

    def attend_to(source, queries, causal):
        scores = lax.dot_general(
            source[:qk_rows], queries, (((0,), (0,)), ((), ())), preferred_element_type=F32
        )
        value = 1.0 + scores * 0.25 + scores * scores * 0.03125
        if causal:
            key_pos = lax.broadcasted_iota(jnp.int32, value.shape, 0)
            query_pos = lax.broadcasted_iota(jnp.int32, value.shape, 1)
            value = jnp.where(key_pos <= query_pos, value, 0.0)
        return jnp.dot(source[qk_rows:], value.astype(BF16), preferred_element_type=F32)

    def attend_own(stack):
        for i in range(2):
            h = 2 * stack + i
            nacc[i] = attend_to(kv[h], q_full[h], True)

    def attend_prior(stack):
        @pl.when(high)
        def _():
            for p in (p_own, p_end):
                kv_copy(p, stack).wait_recv()
            for i in range(2):
                h = 2 * stack + i
                nacc[i] += attend_to(kv_prev[h], q_full[h], False)

        for i in range(2):
            num_send[2 * stack + i] = nacc.at[i][:, lanes(p_end)].astype(BF16)
        launch("inner", num_copy, stack)
        for i in range(2):
            num_all[2 * stack + i, f, s] = nacc.at[i][:, lanes(p_own)].astype(BF16)

    def spread_nums(stack):
        for kind in (1, 0):
            spread_num(stack, kind).start()

    def o_relay(h, pieces_now, inward, cross=True):
        for c in pieces_now:
            o_copy(h, c, False, True).wait_recv()
            if inward is not None:
                o_copy(h, c, False, inward).start()
            if cross and not (inward and c >= out_pieces - whole_pieces):
                across(h, c).start()

    def w_relay(c):
        w_copy(sl_out, c).wait_recv()
        w_copy(sl_out, c).start()

    head_width = 2 * num_all.shape[3]
    columns = out_ref.shape[1]
    depth = 2 * head_width

    def attend_block(h):
        for i in range(2):
            whole = jnp.concatenate([num_all[h, j, i] for j in range(2)], 0).astype(F32)
            meansq = jnp.sum(whole * whole, axis=0, keepdims=True) / head_width
            scaled = (whole * lax.rsqrt(meansq + 1e-06)).T * head_gain_ref[...]
            attended[h, :, i * head_width : (i + 1) * head_width] = scaled.astype(BF16)

    def out_copy(r):
        block = part_rows(r)
        return pltpu.make_async_copy(out_ref.at[block], out_hbm.at[block], out_sem.at[r])

    def multiply(h):
        def add(weights):
            weights = weights.reshape(depth, columns)
            if h == 0:
                total[...] = jnp.dot(attended[h], weights, preferred_element_type=F32)
            elif h < n - 1:
                total[...] += jnp.dot(attended[h], weights, preferred_element_type=F32)
            else:
                for r in range(row_chunks):
                    block = part_rows(r)
                    product = jnp.dot(attended[h, block], weights, preferred_element_type=F32)
                    out_ref[block] = (total[block] + product).astype(BF16)
                    out_copy(r).start()

        @pl.when(my == h)
        def _():
            add(wo_ref[...])

        @pl.when(my != h)
        def _():
            crossed(h)
            add(wobuf[h])

    late = range(early, out_pieces)
    def far_w(c):
        w_copy(sl_far, c).wait_recv()

    @pl.when(inner)
    def _():
        for c in range(out_pieces):
            o_copy(my, c, True, True).start()
        o_relay(sl_out, range(early), True)
        gather_own(0, 0)
        gather_own(1, 0)
        gather_own(0, 1)
        gather_fwd(0, 0)
        gather_own(1, 1)
        gather_own(0, 2)
        gather_fwd(1, 0)
        gather_own(1, 2)
        gather_own(0, 3)
        for c in range(w_pieces):
            w_copy(second, c).wait_recv()
        project(3, 0, 0, w_pieces, True)
        send_qk(3, 0)
        gather_fwd(0, 1)
        gather_own(1, 3)
        gather_fwd(0, 2)
        o_relay(second, (0, 1), False)
        gather_fwd(1, 1)
        gather_own(2, 0)
        gather_fwd(0, 3)
        o_relay(second, (2, 3), False)
        gather_fwd(1, 2)
        gather_own(2, 1)
        o_relay(second, (4, 5), False)
        gather_fwd(1, 3)
        gather_own(2, 2)
        gathered(0, (q_sib, q_diag))
        project(0, 0, 0, w_pieces, True)
        pl.semaphore_wait(beyond, 1)
        send_part(0, 0)
        o_relay(second, (6, 7), False)
        gather_fwd(2, 0)
        gather_own(2, 3)
        gathered(1, (q_sib, q_diag))
        project(1, 0, 0, w_pieces, True)
        send_qk(1, 0)
        o_relay(sl_far, range(early), False)
        gather_fwd(2, 1)
        w_relay(0)
        w_relay(1)
        gather_fwd(2, 2)
        w_relay(2)
        w_relay(3)
        gather_fwd(2, 3)
        gathered(2, (q_sib, q_diag))
        project(2, 0, 0, w_pieces, True)
        send_part(2, 0)
        w_relay(4)
        w_relay(5)
        far_w(0)
        far_w(1)
        for k in range(4):
            project(k, 1, 0, 2, True)
        w_relay(6)
        far_w(2)
        far_w(3)
        for k in range(4):
            project(k, 1, 2, 4, False)
        w_relay(7)
        finish_proj(0, True)
        far_w(4)
        far_w(5)
        for k in range(4):
            project(k, 1, 4, 6, False)
        finish_proj(0, False)
        o_relay(sl_out, (early, early + 1), True, False)
        far_w(6)
        o_relay(sl_out, (early + 2,), True, False)
        far_w(7)
        for k in (2, 0):
            project(k, 1, 6, w_pieces, False)
            send_part(k, 1)
        for c in range(early, min(early + 3, out_pieces - whole_pieces)):
            across(sl_out, c).start()
        for k in (1, 3):
            project(k, 1, 6, w_pieces, False)
            send_qk(k, 1)
        o_relay(sl_out, range(early + 3, out_pieces), True)
        attend_own(0)
        o_relay(sl_far, (early, early + 1), False)
        attend_prior(0)
        finish_proj(1, False)
        finish_proj(1, True)
        spread_nums(0)
        o_relay(sl_far, range(early + 2, early + 4), False)
        attend_own(1)

        @pl.when(high)
        def _():
            o_relay(sl_far, range(early + 4, out_pieces), False)

        attend_prior(1)
        spread_nums(1)

        @pl.when(low)
        def _():
            o_relay(sl_far, range(early + 4, out_pieces), False)

        nums_passed(0)
        nums_gathered(0)
        for h in range(2):
            attend_block(h)
            multiply(h)
        nums_passed(1)
        nums_gathered(1)
        for h in range(2, n):
            attend_block(h)
            multiply(h)

    @pl.when(outer)
    def _():
        for r in range(row_chunks):
            tok_arrive(0, quarter, r)
            z_tok(2, r).start()
        for c in range(w_pieces):
            w_loaded(c)
            w_copy(my, c).start()
        for c in late:
            o_copy(my, c, True, True).start()
        for c in range(out_pieces - whole_pieces, out_pieces):
            o_other(c).start()
        o_relay(near, range(out_pieces), None)
        o_relay(second, range(out_pieces), None)
        o_relay(sl_far, range(early), None)
        nums_taken(0)
        o_relay(sl_far, range(early, early + 2), None)
        nums_passed(0)

        @pl.when(low)
        def _():
            o_relay(sl_far, range(early + 2, early + 4), None)
            nums_taken(1)

        nums_gathered(0)
        for h in range(2):
            attend_block(h)
            multiply(h)

        @pl.when(high)
        def _():
            o_relay(sl_far, range(early + 2, out_pieces), None)
            nums_taken(1)

        @pl.when(low)
        def _():
            o_relay(sl_far, range(early + 4, out_pieces), None)

        nums_passed(1)
        nums_gathered(1)
        for h in range(2, n):
            attend_block(h)
            multiply(h)

    def flush(whole, sem):
        remote(whole, whole, sem, sem, {"sub": 1 - s}).wait_send()

    def tok_flush(k, kind):
        flush(xq.at[k, quarter], tok_s.at[k, kind])

    for role, gate in (("inner", inner), ("outer", outer), ("low", inner & low)):

        @pl.when(gate)
        def _():
            for make, args in logs[role]:
                make(*args).wait_send()

    @pl.when(inner)
    def _():
        for h in (my, sl_out):
            flush(wall.at[:, h], w_ss.at[h])
            flush(wobuf.at[h, g], o_in.at[h])
        for h in (my, second, sl_far):
            flush(wobuf.at[h, g], o_out.at[h])
        for h in (second, sl_far):
            flush(wobuf.at[h, g], o_ac.at[h])
        flush(wobuf.at[sl_out, g, pl.ds(0, out_pieces - whole_pieces)], o_ac.at[sl_out])
        for k in range(3):
            for kind in (1, 2, 3):
                tok_flush(k, kind)

    @pl.when(outer)
    def _():
        flush(wall.at[:, my], w_ss.at[my])
        flush(wobuf.at[my, g], o_in.at[my])
        for h in (near, second, sl_far):
            flush(wobuf.at[h, g], o_ac.at[h])
        flush(wobuf.at[my, g, pl.ds(0, whole_pieces)], o_ac.at[my])
        for k in (1, 2):
            tok_flush(k, 0)

    tok_flush(0, 0)
    for stack in range(2):
        for kind in range(3):
            spread_num(stack, kind).wait_send()
    for r in range(row_chunks):
        out_copy(r).wait()


def per_device_line(n, tokens, norm_gain, w_query, w_key, w_value, head_gain, w_out):
    count, width = tokens.shape
    shards = [w_query[0], w_key[0], w_value[0]]
    rows = sum(shard.shape[0] for shard in shards)
    qk_rows = w_query.shape[1] + w_key.shape[1]
    channels = w_value.shape[1]
    head_width, columns = w_out.shape[1], w_out.shape[2]
    pieces, w_pieces, out_pieces, row_chunks = 4, 8, 8, 4
    early, whole_pieces, direct = 3, 3, 2
    span = width // (2 * pieces)
    wo = w_out.reshape(2, out_pieces, head_width // out_pieces, columns)
    hbm = pl.BlockSpec(memory_space=pl.ANY)
    vmem = pl.BlockSpec(memory_space=pltpu.VMEM)
    dma = pltpu.SemaphoreType.DMA
    return pl.pallas_call(
        functools.partial(line_kernel, n, pieces, w_pieces, out_pieces, early, whole_pieces, direct, row_chunks),
        out_shape=jax.ShapeDtypeStruct((count, columns), BF16),
        in_specs=[hbm, vmem, vmem, hbm] + [hbm] * 3,
        out_specs=hbm,
        scratch_shapes=[
            pltpu.VMEM(tokens.shape, BF16),
            pltpu.VMEM(wo.shape, BF16),
            pltpu.VMEM((count, columns), BF16),
            dma((w_pieces + 1 + row_chunks,)),
            dma((row_chunks,)),
            pltpu.VMEM((count, span), BF16),
            pltpu.VMEM((count, span), BF16),
            pltpu.VMEM((pieces, count, span), BF16),
            pltpu.VMEM((3, pieces, count, span), BF16),
            pltpu.VMEM((w_pieces, n, rows, span * pieces // w_pieces), BF16),
            pltpu.VMEM((n,) + wo.shape, BF16),
            pltpu.VMEM((4, n // 2, 2 * rows, count), F32),
            pltpu.VMEM((2, n, rows, count), BF16),
            pltpu.VMEM((2, n, rows, count), BF16),
            pltpu.VMEM((2, 2, n, qk_rows, count), BF16),
            pltpu.VMEM((n, qk_rows, 2 * count), BF16),
            pltpu.VMEM((n, rows, 2 * count), BF16),
            pltpu.VMEM((n, rows, 2 * count), BF16),
            pltpu.VMEM((2, n, qk_rows, count), BF16),
            pltpu.VMEM((2, channels, 2 * count), F32),
            pltpu.VMEM((n, channels, count), BF16),
            pltpu.VMEM((n, 2, 2, channels, count), BF16),
            pltpu.VMEM((n, count, 2 * head_width), BF16),
            pltpu.VMEM((count, columns), F32),
            dma((n,)),
            dma((n, w_pieces)),
            dma((3, 4)),
            dma((3, pieces, row_chunks)),
            dma((n,)),
            dma((n,)),
            dma((n, out_pieces)),
            dma((n,)),
            dma((n,)),
            dma((2, n // 2)),
            dma((2, n // 2)),
            dma((2, n // 2, 2)),
            dma((2, n // 2, 2)),
            dma((2, n // 2)),
            dma((2, n // 2)),
            dma((n // 2,)),
            dma((n // 2, 3)),
            dma((n // 2, 2, 2)),
            pltpu.SemaphoreType.REGULAR,
        ],
        compiler_params=pltpu.CompilerParams(
            collective_id=0, has_side_effects=True, vmem_limit_bytes=60 * 1024 * 1024
        ),
    )(tokens, norm_gain.reshape(1, -1), head_gain.reshape(1, -1), wo, *shards)


def per_device(sizes, tokens, norm_gain, w_query, w_key, w_value, head_gain, w_out):
    n, nf, ns = sizes
    shards = [w_query[0], w_key[0], w_value[0]]
    if any(shard.shape[0] % 8 for shard in shards):
        shards = [jnp.concatenate(shards, 0)]
    rows, width = sum(shard.shape[0] for shard in shards), tokens.shape[1]
    count = tokens.shape[0]
    qk_rows = w_query.shape[1] + w_key.shape[1]
    channels = w_value.shape[1]
    head_width, columns = w_out.shape[1], w_out.shape[2]
    pieces = max(1, 16 // n)
    out_pieces = max(1, 16 // n)
    wo = w_out.reshape(ns, out_pieces, head_width // out_pieces, columns)
    hbm = pl.BlockSpec(memory_space=pl.ANY)
    vmem = pl.BlockSpec(memory_space=pltpu.VMEM)
    dma = pltpu.SemaphoreType.DMA
    return pl.pallas_call(
        functools.partial(kernel, n, nf, ns, pieces, out_pieces, len(shards)),
        out_shape=jax.ShapeDtypeStruct((count, columns), BF16),
        in_specs=[hbm, vmem, vmem, hbm] + [hbm] * len(shards),
        out_specs=vmem,
        scratch_shapes=[
            pltpu.VMEM(tokens.shape, BF16),
            pltpu.VMEM((rows, width), BF16),
            pltpu.VMEM(wo.shape, BF16),
            dma((len(shards) + 2,)),
            pltpu.VMEM((2 * pieces, count, width // (2 * pieces)), BF16),
            pltpu.VMEM((n, 2, pieces, rows, width // (2 * pieces)), BF16),
            pltpu.VMEM((n,) + wo.shape, BF16),
            pltpu.VMEM((n, qk_rows, count), BF16),
            pltpu.VMEM((n, channels, count), BF16),
            pltpu.VMEM((n, nf, qk_rows, count), BF16),
            pltpu.VMEM((n, channels, count), BF16),
            pltpu.VMEM((n, nf * qk_rows // 2, count), BF16),
            pltpu.VMEM((n, nf * qk_rows // 2, count), BF16),
            pltpu.VMEM((n, channels, count), BF16),
            pltpu.VMEM((n, nf, ns, channels, count), BF16),
            pltpu.VMEM((n, count, ns * head_width), BF16),
            pltpu.VMEM((count, columns), F32),
        ]
        + [dma((n, pieces))] * 5
        + [dma((n, out_pieces))] * 5
        + [
            dma((n, nf)),
            dma((n, nf)),
            dma((n,)),
            dma((n,)),
            dma((n,)),
            dma((n,)),
            dma((n, nf, ns)),
            dma((n, nf, ns)),
        ],
        compiler_params=pltpu.CompilerParams(
            collective_id=0, has_side_effects=True, vmem_limit_bytes=60 * 1024 * 1024
        ),
    )(tokens, norm_gain.reshape(1, -1), head_gain.reshape(1, -1), wo, *shards)


def solution(mesh):
    in_specs = (
        P(("groups", "seq"), None),
        P(),
        P(("seq", "sub"), "fsdp", None),
        P(("seq", "sub"), "fsdp", None),
        P(("seq", "sub"), "fsdp", None),
        P(),
        P("seq", None, ("fsdp", "sub")),
    )
    out_specs = P(("groups", "seq"), ("fsdp", "sub"))
    sizes = (mesh.shape["seq"], mesh.shape["fsdp"], mesh.shape["sub"])
    if sizes == (4, 2, 2):
        body = functools.partial(per_device_line, sizes[0])
    else:
        body = functools.partial(per_device, sizes)
    return jax.shard_map(
        body,
        mesh=mesh,
        in_specs=in_specs,
        out_specs=out_specs,
        check_vma=False,
    )
```

```python
import functools

import jax
import jax.numpy as jnp
from jax import lax
from jax.experimental import pallas as pl
from jax.experimental.pallas import tpu as pltpu
from jax.sharding import PartitionSpec as P

MESH = pl.DeviceIdType.MESH
F32 = jnp.float32
BF16 = jnp.bfloat16


def kernel(
    n,
    nf,
    ns,
    pieces,
    out_pieces,
    w_count,
    tok_hbm,
    gain_ref,
    head_gain_ref,
    wo_hbm,
    *rest,
):
    kernel_body(
        n, nf, ns, pieces, out_pieces, tok_hbm, gain_ref, head_gain_ref, wo_hbm,
        rest[:w_count], *rest[w_count:]
    )


def kernel_body(
    n,
    nf,
    ns,
    pieces,
    out_pieces,
    tok_hbm,
    gain_ref,
    head_gain_ref,
    wo_hbm,
    w_hbm,
    out_ref,
    tok_ref,
    w_ref,
    wo_ref,
    load_sem,
    normed,
    wbuf,
    wobuf,
    qk_send,
    v_send,
    qk_all,
    v_all,
    q_full,
    k_full,
    num_send,
    num_all,
    attended,
    total,
    w_zrecv,
    w_yrecv,
    w_right,
    w_left,
    w_across,
    o_zrecv,
    o_yrecv,
    o_right,
    o_left,
    o_across,
    qk_ssem,
    qk_rsem,
    v_ssem,
    v_rsem,
    num_ssem,
    num_rsem,
    sib_ssem,
    sib_rsem,
):
    group = lax.axis_index("groups")
    me = lax.axis_index("seq")
    my_f = lax.axis_index("fsdp")
    my_s = lax.axis_index("sub")
    tokens, width = tok_ref.shape

    loads = []
    row = 0
    for k, source in enumerate(w_hbm):
        size = source.shape[0]
        target = w_ref.at[pl.ds(row, size)] if len(w_hbm) > 1 else w_ref
        loads.append(pltpu.make_async_copy(source, target, load_sem.at[k]))
        row += size
    tok_load = pltpu.make_async_copy(tok_hbm, tok_ref, load_sem.at[len(w_hbm)])
    wo_load = pltpu.make_async_copy(wo_hbm, wo_ref, load_sem.at[len(w_hbm) + 1])
    for load in loads + [tok_load, wo_load]:
        load.start()

    peers = [
        {"seq": lax.rem(me + dz, n), "fsdp": lax.rem(my_f + df, nf)}
        for dz in range(n)
        for df in range(nf)
        if dz or df
    ]
    peers += [
        {"fsdp": lax.rem(my_f + df, nf), "sub": lax.rem(my_s + ds, ns)}
        for df in range(nf)
        for ds in range(1, ns)
    ]
    peers += [{"groups": 1 - group}]
    barrier = pltpu.get_barrier_semaphore()
    for peer in peers:
        pl.semaphore_signal(barrier, inc=1, device_id=peer, device_id_type=MESH)
    pl.semaphore_wait(barrier, len(peers))
    for load in loads:
        load.wait()
    span = width // (2 * pieces)
    qk_rows = qk_all.shape[2]
    half_rows = qk_rows // 2

    def own_w(c):
        start = pl.multiple_of((group * pieces + c) * span, span)
        return w_ref.at[:, pl.ds(start, span)]

    def own_o(c):
        return wo_ref.at[group, c]

    class Stream:
        def __init__(self, own, buf, count, zrecv, yrecv, right, left, across):
            self.own, self.buf, self.count = own, buf, count
            self.zrecv, self.yrecv = zrecv, yrecv
            self.right_sem, self.left_sem, self.across_sem = right, left, across

        def along(self, o, c, sems, target, own):
            slot = self.buf.at[o, group, c]
            return pltpu.make_async_remote_copy(
                src_ref=self.own(c) if own else slot,
                dst_ref=slot,
                send_sem=sems.at[o, c],
                recv_sem=self.zrecv.at[o, c],
                device_id={"seq": target},
                device_id_type=MESH,
            )

        def right(self, o, c, own=False):
            return self.along(o, c, self.right_sem, me + 1, own)

        def left(self, o, c, own=False):
            return self.along(o, c, self.left_sem, me - 1, own)

        def across(self, o, c, half):
            slot = self.buf.at[o, half, c]
            return pltpu.make_async_remote_copy(
                src_ref=slot,
                dst_ref=slot,
                send_sem=self.across_sem.at[o, c],
                recv_sem=self.yrecv.at[o, c],
                device_id={"groups": 1 - group},
                device_id_type=MESH,
            )

        def begin(self):
            for c in range(self.count):

                @pl.when(me + 1 < n)
                def _():
                    self.right(me, c, True).start()

                @pl.when(me >= 1)
                def _():
                    self.left(me, c, True).start()

        def relay(self, r, between=None):
            for c in range(self.count):
                if between is not None and c == self.count // 2:
                    between()

                @pl.when(me >= r)
                def _():
                    o = me - r
                    self.right(o, c).wait_recv()

                    @pl.when(me + 1 < n)
                    def _():
                        self.right(o, c).start()

                    self.across(o, c, group).start()

                @pl.when(me + r < n)
                def _():
                    o = me + r
                    self.left(o, c).wait_recv()

                    @pl.when(me >= 1)
                    def _():
                        self.left(o, c).start()

                    self.across(o, c, group).start()

        def arrive(self, o):
            for c in range(self.count):
                self.across(o, c, 1 - group).wait_recv()

        def finish(self):
            for r in range(n):
                for c in range(self.count):

                    @pl.when((me >= r) & (me + 1 < n))
                    def _():
                        self.right(me - r, c, r == 0).wait_send()

                    @pl.when((me + r < n) & (me >= 1))
                    def _():
                        self.left(me + r, c, r == 0).wait_send()

                    if r > 0:

                        @pl.when(me >= r)
                        def _():
                            self.across(me - r, c, group).wait_send()

                        @pl.when(me + r < n)
                        def _():
                            self.across(me + r, c, group).wait_send()

    w_stream = Stream(own_w, wbuf, pieces, w_zrecv, w_yrecv, w_right, w_left, w_across)
    o_stream = Stream(own_o, wobuf, out_pieces, o_zrecv, o_yrecv, o_right, o_left, o_across)

    w_stream.begin()
    wo_load.wait()
    at_end = (me == 0) | (me == n - 1)

    @pl.when(at_end)
    def _():
        o_stream.begin()

    tok_load.wait()

    row_step = 16

    def norm_rows(i, carry):
        rows = pl.ds(pl.multiple_of(i * row_step, row_step), row_step)
        sumsq = jnp.zeros((row_step, 1), F32)
        for c in range(2 * pieces):
            part = tok_ref[rows, c * span : (c + 1) * span].astype(F32)
            sumsq = sumsq + jnp.sum(part * part, axis=1, keepdims=True)
        scale = lax.rsqrt(sumsq / width + 1e-05)
        for c in range(2 * pieces):
            cols = slice(c * span, (c + 1) * span)
            part = tok_ref[rows, cols].astype(F32)
            normed[c, rows, :] = (part * scale * gain_ref[:, cols]).astype(BF16)
        return carry

    lax.fori_loop(0, tokens // row_step, norm_rows, 0)

    def contract(weights, acts):
        return lax.dot_general(weights, acts, (((1,), (1,)), ((), ())), preferred_element_type=F32)

    def qk_copy(o, source, other_f, token_block, f_from):
        return pltpu.make_async_remote_copy(
            src_ref=source,
            dst_ref=qk_all.at[token_block, f_from],
            send_sem=qk_ssem.at[o, other_f],
            recv_sem=qk_rsem.at[token_block, f_from],
            device_id={"seq": o, "fsdp": other_f},
            device_id_type=MESH,
        )

    def v_copy(o, token_block):
        return pltpu.make_async_remote_copy(
            src_ref=v_send.at[o],
            dst_ref=v_all.at[token_block],
            send_sem=v_ssem.at[o],
            recv_sem=v_rsem.at[token_block],
            device_id={"seq": o},
            device_id_type=MESH,
        )

    def project_own():
        acc = jnp.zeros((w_ref.shape[0], tokens), F32)
        for c in range(2 * pieces):
            acc = acc + contract(w_ref[:, c * span : (c + 1) * span], normed[c])
        qk_all[me, my_f] = acc[:qk_rows].astype(BF16)
        v_all[me] = acc[qk_rows:].astype(BF16)
        for df in range(1, nf):
            other = lax.rem(my_f + df, nf)
            qk_copy(me, qk_all.at[me, my_f], other, me, my_f).start()

    def project(o):
        def body(c, acc):
            return acc + contract(wbuf[o, c // pieces, c % pieces], normed[c])

        acc = lax.fori_loop(0, 2 * pieces, body, jnp.zeros((w_ref.shape[0], tokens), F32))
        qk_send[o] = acc[:qk_rows].astype(BF16)
        v_send[o] = acc[qk_rows:].astype(BF16)
        for df in range(nf):
            qk_copy(o, qk_send.at[o], lax.rem(my_f + df, nf), me, my_f).start()
        v_copy(o, me).start()

    def both(r, action):
        @pl.when(me >= r)
        def _():
            action(me - r)

        @pl.when(me + r < n)
        def _():
            action(me + r)

    def take(o):
        w_stream.arrive(o)
        project(o)

    project_own()
    for r in range(1, n):
        if r == n - 1:

            @pl.when(jnp.logical_not(at_end))
            def _():
                o_stream.begin()

        w_stream.relay(r, functools.partial(both, r - 1, take) if r > 1 else None)

    o_stream.relay(1, functools.partial(both, n - 1, take))

    def gather_heads():
        for d in range(1, n):
            t = lax.rem(me + d, n)
            v_copy(me, t).wait_recv()
            for df in range(nf):
                qk_copy(me, qk_all.at[t, df], 0, t, df).wait_recv()
        for df in range(1, nf):
            other = lax.rem(my_f + df, nf)
            qk_copy(me, qk_all.at[me, other], other, me, other).wait_recv()

        for t in range(n):
            parts = [qk_all[t, f].astype(F32) for f in range(nf)]
            q_full[t] = jnp.concatenate([p[:half_rows] for p in parts], 0).astype(BF16)
            k_full[t] = jnp.concatenate([p[half_rows:] for p in parts], 0).astype(BF16)

    channels = v_all.shape[1]
    key_pos = lax.broadcasted_iota(jnp.int32, (tokens, tokens), 0)
    query_pos = lax.broadcasted_iota(jnp.int32, (tokens, tokens), 1)

    def numerator(t):
        queries = q_full[t]

        def body(j, acc):
            scores = lax.dot_general(
                k_full[j], queries, (((0,), (0,)), ((), ())), preferred_element_type=F32
            )
            value = 1.0 + scores * 0.25 + scores * scores * 0.03125
            weight = jnp.where(key_pos + (j - t) * tokens <= query_pos, value, 0.0).astype(BF16)
            return acc + jnp.dot(v_all[j], weight, preferred_element_type=F32)

        acc = lax.fori_loop(0, t + 1, body, jnp.zeros((channels, tokens), F32))
        return acc.astype(BF16)

    def num_copy(t, head_block):
        return pltpu.make_async_remote_copy(
            src_ref=num_send.at[t],
            dst_ref=num_all.at[head_block, my_f, my_s],
            send_sem=num_ssem.at[t],
            recv_sem=num_rsem.at[head_block],
            device_id={"seq": t},
            device_id_type=MESH,
        )

    def sib_copy(o, to_f, to_s, from_f, from_s):
        slot = num_all.at[o, from_f, from_s]
        return pltpu.make_async_remote_copy(
            src_ref=slot,
            dst_ref=slot,
            send_sem=sib_ssem.at[o, to_f, to_s],
            recv_sem=sib_rsem.at[o, from_f, from_s],
            device_id={"fsdp": to_f, "sub": to_s},
            device_id_type=MESH,
        )

    def siblings():
        for df in range(nf):
            for ds in range(ns):
                if df or ds:
                    yield lax.rem(my_f + df, nf), lax.rem(my_s + ds, ns)

    def attend():
        gather_heads()
        for d in range(1, n):
            t = lax.rem(me + d, n)
            num_send[t] = numerator(t)
            num_copy(t, me).start()
        num_all[me, my_f, my_s] = numerator(me)
        for f, s in siblings():
            sib_copy(me, f, s, my_f, my_s).start()

    def spread():
        for d in range(1, n):
            o = lax.rem(me + d, n)
            num_copy(o, o).wait_recv()
            for f, s in siblings():
                sib_copy(o, f, s, my_f, my_s).start()

    for r in range(2, n):
        o_stream.relay(r, {2: attend, 3: spread}.get(r))

    for d in range(n):
        o = lax.rem(me + d, n)
        for f, s in siblings():
            sib_copy(o, f, s, f, s).wait_recv()

    head_width = nf * channels

    def attend_block(o, carry):
        for s in range(ns):
            whole = jnp.concatenate([num_all[o, f, s] for f in range(nf)], 0).astype(F32)
            meansq = jnp.sum(whole * whole, axis=0, keepdims=True) / head_width
            scaled = (whole * lax.rsqrt(meansq + 1e-06)).T * head_gain_ref[...]
            attended[o, :, s * head_width : (s + 1) * head_width] = scaled.astype(BF16)
        return carry

    lax.fori_loop(0, n, attend_block, 0)

    columns = out_ref.shape[1]
    depth = ns * head_width

    total[...] = jnp.dot(
        attended[me], wo_ref[...].reshape(depth, columns), preferred_element_type=F32
    )

    def multiply(o):
        o_stream.arrive(o)
        total[...] += jnp.dot(
            attended[o], wobuf[o].reshape(depth, columns), preferred_element_type=F32
        )

    for r in range(1, n):
        both(r, multiply)
    out_ref[...] = total[...].astype(BF16)

    w_stream.finish()
    o_stream.finish()
    for d in range(n):
        o = lax.rem(me + d, n)
        for df in range(nf):
            if d or df:
                other = lax.rem(my_f + df, nf)
                source = qk_send.at[o] if d else qk_all.at[me, my_f]
                qk_copy(o, source, other, me, my_f).wait_send()
        if d:
            v_copy(o, me).wait_send()
            num_copy(o, me).wait_send()
        for f, s in siblings():
            sib_copy(o, f, s, my_f, my_s).wait_send()

def line_kernel(
    n,
    pieces,
    w_pieces,
    out_pieces,
    early,
    whole_pieces,
    direct,
    row_chunks,
    tok_hbm,
    gain_ref,
    head_gain_ref,
    wo_hbm,
    wq_hbm,
    wk_hbm,
    wv_hbm,
    out_hbm,
    tok_ref,
    wo_ref,
    out_ref,
    load_sem,
    out_sem,
    ysend,
    ysend2,
    xn,
    xq,
    wall,
    wobuf,
    acc,
    part_send,
    part_recv,
    qk,
    q_full,
    kv,
    state,
    state_in,
    feats,
    qk_mine,
    nacc,
    num_send,
    num_all,
    attended,
    total,
    w_ss,
    w_rs,
    tok_s,
    tok_r,
    o_out,
    o_in,
    o_rs,
    o_ac,
    o_yr,
    part_s,
    part_r,
    qk_s,
    qk_r,
    kv_s,
    kv_r,
    num_s,
    ng_s,
    ng_r,
    beyond,
):
    g = lax.axis_index("groups")
    z = lax.axis_index("seq")
    f = lax.axis_index("fsdp")
    s = lax.axis_index("sub")
    upper = z // (n // 2)
    sign = 2 * upper - 1
    out_z = z + sign
    in_z = z - sign
    inner = (z > 0) & (z < n - 1)
    outer = jnp.logical_not(inner)
    low = upper == 0
    high = upper == 1
    near = upper
    second = 1 - upper
    ends = n - 2
    my = jnp.where(inner, upper, ends + upper)
    sl_out = ends + upper
    sl_far = ends + 1 - upper
    p_own = 1 - upper
    p_end = upper
    tokens, width = tok_ref.shape
    rows, w_span = wall.shape[2], wall.shape[3]
    span = xn.shape[2]
    split = span // w_span
    qk_rows = qk.shape[3]
    half_rows = qk_rows // 2
    quarter = f * 2 + s
    f_other = 1 - f
    q_sib = f * 2 + 1 - s
    q_x = (1 - f) * 2 + s
    q_diag = (1 - f) * 2 + 1 - s

    loads = []
    for c in range(w_pieces):
        row = 0
        for source in (wq_hbm, wk_hbm, wv_hbm):
            size = source.shape[0]
            col = pl.multiple_of((g * w_pieces + c) * w_span, w_span)
            loads.append(
                pltpu.make_async_copy(
                    source.at[:, pl.ds(col, w_span)],
                    wall.at[c, my, pl.ds(row, size)],
                    load_sem.at[c],
                )
            )
            row += size

    def w_loaded(c):
        slot = wall.at[c, my]
        pltpu.make_async_copy(slot, slot, load_sem.at[c]).wait()

    wo_load = pltpu.make_async_copy(wo_hbm, wo_ref, load_sem.at[w_pieces])
    step = tokens // row_chunks
    tok_loads = [
        pltpu.make_async_copy(
            tok_hbm.at[pl.ds(r * step, step)],
            tok_ref.at[pl.ds(r * step, step)],
            load_sem.at[w_pieces + 1 + r],
        )
        for r in range(row_chunks)
    ]
    for load in loads + [wo_load] + tok_loads:
        load.start()

    barrier = pltpu.get_barrier_semaphore()
    for peer in (
        {"seq": in_z},
        {"groups": 1 - g},
        {"fsdp": 1 - f},
        {"sub": 1 - s},
    ):
        pl.semaphore_signal(barrier, inc=1, device_id=peer, device_id_type=MESH)

    @pl.when(inner)
    def _():
        pl.semaphore_signal(barrier, inc=1, device_id={"seq": out_z}, device_id_type=MESH)
        pl.semaphore_wait(barrier, 5)
        pl.semaphore_signal(beyond, inc=1, device_id={"fsdp": 1 - f}, device_id_type=MESH)

    @pl.when(outer)
    def _():
        pl.semaphore_wait(barrier, 4)

    logs = {"inner": [], "outer": [], "all": [], "low": []}

    def launch(role, make, *args):
        make(*args).start()
        logs[role].append((make, args))

    def remote(src, dst, send, recv, to):
        return pltpu.make_async_remote_copy(
            src_ref=src,
            dst_ref=dst,
            send_sem=send,
            recv_sem=recv,
            device_id=to,
            device_id_type=MESH,
        )

    def w_copy(h, c):
        slot = wall.at[c, h]
        return remote(slot, slot, w_ss.at[h], w_rs.at[h, c], {"seq": in_z})

    def o_copy(h, c, own, inward):
        slot = wobuf.at[h, g, c]
        return remote(
            wo_ref.at[g, c] if own else slot,
            slot,
            (o_in if inward else o_out).at[h],
            o_rs.at[h, c],
            {"seq": in_z if inward else out_z},
        )

    def o_other(c):
        return remote(
            wo_ref.at[1 - g, c], wobuf.at[my, 1 - g, c], o_ac.at[my], o_yr.at[my], {"seq": in_z}
        )

    def across(h, c):
        slot = wobuf.at[h, g, c]
        return remote(slot, slot, o_ac.at[h], o_yr.at[h], {"groups": 1 - g})

    def crossed(h):
        slot = wobuf.at[h, 1 - g]
        remote(slot, slot, o_ac.at[h], o_yr.at[h], {"groups": 1 - g}).wait_recv()

    def part_rows(r):
        return pl.ds(r * step, step)

    def y_tok(r):
        return remote(
            ysend.at[part_rows(r)],
            xq.at[0, quarter, part_rows(r)],
            tok_s.at[0, 0],
            tok_r.at[0, quarter, r],
            {"groups": 1 - g},
        )

    def y_tok2(r):
        return remote(
            ysend2.at[part_rows(r)],
            xq.at[0, q_x, part_rows(r)],
            tok_s.at[0, 2],
            tok_r.at[0, q_x, r],
            {"groups": 1 - g},
        )

    def z_tok(k, r):
        src = xn.at[quarter, part_rows(r)] if k == 1 else xq.at[0, quarter, part_rows(r)]
        return remote(
            src,
            xq.at[k, quarter, part_rows(r)],
            tok_s.at[k, 0],
            tok_r.at[k, quarter, r],
            {"seq": in_z},
        )

    def spread_tok(k, c, r, kind):
        slot = xq.at[k, c, part_rows(r)]
        to = {"fsdp": 1 - f} if kind == 2 else {"sub": 1 - s}
        return remote(slot, slot, tok_s.at[k, kind], tok_r.at[k, c, r], to)

    def tok_arrive(k, c, r):
        slot = xq.at[k, c, part_rows(r)]
        remote(slot, slot, tok_s.at[k, 1], tok_r.at[k, c, r], {"sub": 1 - s}).wait_recv()

    def gather_own(k, r):
        tok_arrive(k, quarter, r)
        if k > 0 or r < direct:
            spread_tok(k, quarter, r, 2).start()
        spread_tok(k, quarter, r, 1).start()

    def gather_fwd(k, r):
        tok_arrive(k, q_x, r)
        spread_tok(k, q_x, r, 3).start()

    def gathered(k, which):
        for r in range(row_chunks):
            for c in which:
                tok_arrive(k, c, r)

    def both(stack):
        return pl.ds(2 * stack, 2)

    def part_copy(p, stack):
        return remote(
            part_send.at[p, both(stack)],
            part_recv.at[p, both(stack)],
            part_s.at[p, stack],
            part_r.at[p, stack],
            {"groups": 1 - g},
        )

    def qk_copy(p, stack, way):
        if way:
            src = part_send.at[p, both(stack), pl.ds(0, qk_rows)]
            to = {"groups": 1 - g, "fsdp": 1 - f}
        else:
            src, to = qk_mine.at[p, both(stack)], {"fsdp": 1 - f}
        return remote(
            src, qk.at[p, way, both(stack)], qk_s.at[p, stack, way], qk_r.at[p, stack, way], to
        )

    def lanes(p):
        start = p * tokens
        return pl.ds(start if isinstance(p, int) else pl.multiple_of(start, tokens), tokens)

    def state_copy(stack):
        return remote(
            state.at[both(stack)],
            state_in.at[both(stack)],
            kv_s.at[stack],
            kv_r.at[stack],
            {"seq": in_z},
        )

    def num_copy(stack):
        return remote(
            num_send.at[both(stack)],
            num_all.at[both(stack), f, s],
            num_s.at[stack],
            ng_r.at[stack, f, s],
            {"seq": out_z},
        )

    def spread_num(stack, kind):
        ff = f_other if kind == 2 else f
        slot = num_all.at[both(stack), ff, s]
        to = {"fsdp": 1 - f} if kind == 1 else {"sub": 1 - s}
        return remote(slot, slot, ng_s.at[stack, kind], ng_r.at[stack, ff, s], to)

    def num_arrive(stack, ff, ss):
        slot = num_all.at[both(stack), ff, ss]
        remote(slot, slot, ng_s.at[stack, 0], ng_r.at[stack, ff, ss], {"sub": 1 - s}).wait_recv()

    def nums_taken(stack):
        num_arrive(stack, f, s)
        for kind in (1, 0):
            spread_num(stack, kind).start()

    def nums_passed(stack):
        num_arrive(stack, 1 - f, s)
        spread_num(stack, 2).start()

    def nums_gathered(stack):
        num_arrive(stack, f, 1 - s)
        num_arrive(stack, 1 - f, 1 - s)

    @pl.when(inner)
    def _():
        for c in range(w_pieces):
            w_loaded(c)
            w_copy(my, c).start()
        wo_load.wait()
        for c in range(out_pieces):
            o_copy(my, c, True, False).start()

    @pl.when(outer)
    def _():
        wo_load.wait()
        for c in range(early):
            o_copy(my, c, True, True).start()

    row_step = 16

    def norm_rows(i, carry):
        block = pl.ds(pl.multiple_of(i * row_step, row_step), row_step)
        sumsq = jnp.zeros((row_step, 1), F32)
        for c in range(2 * pieces):
            part = tok_ref[block, c * span : (c + 1) * span].astype(F32)
            sumsq = sumsq + jnp.sum(part * part, axis=1, keepdims=True)
        scale = lax.rsqrt(sumsq / width + 1e-05)

        def column(c):
            cols = pl.ds(pl.multiple_of(c * span, span), span)
            part = tok_ref[block, cols].astype(F32)
            return (part * scale * gain_ref[:, cols]).astype(BF16)

        ysend[block, :] = column((1 - g) * pieces + quarter)
        ysend2[block, :] = column((1 - g) * pieces + q_x)
        for c in range(pieces):
            xn[c, block, :] = column(g * pieces + c)
        return carry

    per_chunk = step // row_step
    for r in range(row_chunks):
        tok_loads[r].wait()
        lax.fori_loop(r * per_chunk, (r + 1) * per_chunk, norm_rows, 0)
        y_tok(r).start()

        @pl.when(outer)
        def _():
            z_tok(1, r).start()

    @pl.when(inner)
    def _():
        for r in range(direct, row_chunks):
            y_tok2(r).start()

    def contract(weights, acts):
        return lax.dot_general(weights, acts, (((1,), (1,)), ((), ())), preferred_element_type=F32)

    def project(k, stack, lo, hi, fresh):
        if fresh:
            acc[k, stack] = jnp.zeros(acc.shape[2:], F32)

        def dot(j, i):
            weights = wall[j * split + i, 2 * stack : 2 * stack + 2].reshape(2 * rows, w_span)
            where = pl.ds(i * w_span, w_span)
            return contract(weights, xn[j, :, where] if k == 3 else xq[k, j, :, where])

        def body(j, carry):
            acc[k, stack] += sum([dot(j, i) for i in range(1, split)], dot(j, 0))
            return carry

        lax.fori_loop(lo // split, hi // split, body, 0)

    def send_part(k, stack):
        p = p_own if k == 0 else p_end
        for i in range(2):
            part_send[p, 2 * stack + i] = acc[k, stack, i * rows : (i + 1) * rows].astype(BF16)
        launch("inner", qk_copy, p, stack, 1)
        launch("inner", part_copy, p, stack)

    def send_qk(k, stack):
        p = p_own if k == 3 else p_end
        for i in range(2):
            part = acc[k, stack, i * rows : i * rows + qk_rows]
            qk_mine[p, 2 * stack + i] = part.astype(BF16)
        launch("inner", qk_copy, p, stack, 0)

    def finish_proj(stack, own):
        p, k = (p_own, 3) if own else (p_end, 1)
        part_copy(p, stack).wait_recv()
        for way in range(2):
            qk_copy(p, stack, way).wait_recv()
        for i in range(2):
            h = 2 * stack + i
            whole = acc[k, stack, i * rows : (i + 1) * rows] + part_recv[p, h].astype(F32)
            mine = whole[:qk_rows].astype(BF16).astype(F32)
            other = qk[p, 0, h].astype(F32) + qk[p, 1, h].astype(F32)
            lower = jnp.where(f == 0, mine, other)
            higher = jnp.where(f == 0, other, mine)

            def joined(first):
                last = first + half_rows
                return jnp.concatenate([lower[first:last], higher[first:last]], 0).astype(BF16)

            q_full[h, pl.ds(0, qk_rows), lanes(p)] = joined(0)
            kv[h, pl.ds(0, qk_rows), lanes(p)] = joined(half_rows)
            kv[h, pl.ds(qk_rows, rows - qk_rows), lanes(p)] = whole[qk_rows:].astype(BF16)

    def attend_to(source, queries, causal):
        scores = lax.dot_general(
            source[:qk_rows], queries, (((0,), (0,)), ((), ())), preferred_element_type=F32
        )
        value = 1.0 + scores * 0.25 + scores * scores * 0.03125
        if causal:
            key_pos = lax.broadcasted_iota(jnp.int32, value.shape, 0)
            query_pos = lax.broadcasted_iota(jnp.int32, value.shape, 1)
            value = jnp.where(key_pos <= query_pos, value, 0.0)
        return jnp.dot(source[qk_rows:], value.astype(BF16), preferred_element_type=F32)

    dims = qk_rows
    sub = dims // 2
    used = sub * dims + sub * sub + dims

    def features(vectors):
        x = vectors.astype(F32)
        parts = [x * x[i : i + 1] for i in range(sub)]
        parts += [x[sub:] * x[i : i + 1] for i in range(sub, dims)]
        rest = (feats.shape[1] - used, x.shape[1])
        one = lax.broadcasted_iota(jnp.int32, rest, 0) == 0
        return jnp.concatenate(parts + [x, jnp.where(one, 1.0, 0.0)], 0).astype(BF16)

    def send_state(stack):
        @pl.when(low)
        def _():
            col = lax.broadcasted_iota(jnp.int32, (1, state.shape[2]), 1)
            twice = (col < sub * dims) & (col % dims >= sub)
            factor = jnp.where(twice, 0.0625, 0.03125)
            factor = jnp.where(col >= used - dims, 0.25, factor)
            factor = jnp.where(col >= used, 1.0, factor)
            for h in range(2 * stack, 2 * stack + 2):
                block = kv[h]
                sums = contract(block[qk_rows:], features(block[:qk_rows]))
                state[h] = (sums * factor).astype(BF16)
            launch("low", state_copy, stack)

    def attend_own(stack):
        @pl.when(high)
        def _():
            for i in range(2):
                feats[i] = features(q_full[2 * stack + i])

        for i in range(2):
            h = 2 * stack + i
            nacc[i] = attend_to(kv[h], q_full[h], True)

    def attend_prior(stack):
        @pl.when(high)
        def _():
            state_copy(stack).wait_recv()
            for i in range(2):
                h = 2 * stack + i
                nacc[i] += jnp.dot(state_in[h], feats[i], preferred_element_type=F32)

        for i in range(2):
            num_send[2 * stack + i] = nacc.at[i][:, lanes(p_end)].astype(BF16)
        launch("inner", num_copy, stack)
        for i in range(2):
            num_all[2 * stack + i, f, s] = nacc.at[i][:, lanes(p_own)].astype(BF16)

    def spread_nums(stack):
        for kind in (1, 0):
            spread_num(stack, kind).start()

    def o_relay(h, pieces_now, inward, cross=True):
        for c in pieces_now:
            o_copy(h, c, False, True).wait_recv()
            if inward is not None:
                o_copy(h, c, False, inward).start()
            if cross and not (inward and c >= out_pieces - whole_pieces):
                across(h, c).start()

    def w_relay(c):
        w_copy(sl_out, c).wait_recv()
        w_copy(sl_out, c).start()

    head_width = 2 * num_all.shape[3]
    columns = out_ref.shape[1]
    depth = 2 * head_width

    def attend_block(h):
        for i in range(2):
            whole = jnp.concatenate([num_all[h, j, i] for j in range(2)], 0).astype(F32)
            meansq = jnp.sum(whole * whole, axis=0, keepdims=True) / head_width
            scaled = (whole * lax.rsqrt(meansq + 1e-06)).T * head_gain_ref[...]
            attended[h, :, i * head_width : (i + 1) * head_width] = scaled.astype(BF16)

    out_span = columns // row_chunks

    def out_copy(r):
        block = pl.ds(r * out_span, out_span)
        return pltpu.make_async_copy(out_ref.at[:, block], out_hbm.at[:, block], out_sem.at[r])

    def multiply(h, own, first=False, last=False):
        attend_block(h)
        if not own:
            crossed(h)
        weights = (wo_ref[...] if own else wobuf[h]).reshape(depth, columns)
        if first:
            total[...] = jnp.dot(attended[h], weights, preferred_element_type=F32)
        elif not last:
            total[...] += jnp.dot(attended[h], weights, preferred_element_type=F32)
        else:
            for r in range(row_chunks):
                block = slice(r * out_span, (r + 1) * out_span)
                product = jnp.dot(attended[h], weights[:, block], preferred_element_type=F32)
                out_ref[:, block] = (total[:, block] + product).astype(BF16)
                out_copy(r).start()

    late = range(early, out_pieces)
    def far_w(c):
        w_copy(sl_far, c).wait_recv()

    @pl.when(inner)
    def _():
        for c in range(out_pieces):
            o_copy(my, c, True, True).start()
        o_relay(sl_out, range(early), True)
        gather_own(0, 0)
        gather_own(1, 0)
        gather_own(0, 1)
        gather_fwd(0, 0)
        gather_own(1, 1)
        gather_own(0, 2)
        gather_fwd(1, 0)
        gather_own(1, 2)
        gather_own(0, 3)
        for c in range(w_pieces):
            w_copy(second, c).wait_recv()
        project(3, 0, 0, w_pieces, True)
        send_qk(3, 0)
        gather_fwd(0, 1)
        gather_own(1, 3)
        gather_fwd(0, 2)
        o_relay(second, (0, 1), False)
        gather_fwd(1, 1)
        gather_own(2, 0)
        gather_fwd(0, 3)
        o_relay(second, (2, 3), False)
        gather_fwd(1, 2)
        gather_own(2, 1)
        o_relay(second, (4, 5), False)
        gather_fwd(1, 3)
        gather_own(2, 2)
        gathered(0, (q_sib, q_diag))
        project(0, 0, 0, w_pieces, True)
        pl.semaphore_wait(beyond, 1)
        send_part(0, 0)
        o_relay(second, (6, 7), False)
        gather_fwd(2, 0)
        gather_own(2, 3)
        gathered(1, (q_sib, q_diag))
        project(1, 0, 0, w_pieces, True)
        send_qk(1, 0)
        o_relay(sl_far, range(early), False)
        gather_fwd(2, 1)
        w_relay(0)
        w_relay(1)
        gather_fwd(2, 2)
        w_relay(2)
        w_relay(3)
        gather_fwd(2, 3)
        gathered(2, (q_sib, q_diag))
        project(2, 0, 0, w_pieces, True)
        send_part(2, 0)
        w_relay(4)
        w_relay(5)
        far_w(0)
        far_w(1)
        for k in range(4):
            project(k, 1, 0, 2, True)
        w_relay(6)
        far_w(2)
        far_w(3)
        for k in range(4):
            project(k, 1, 2, 4, False)
        w_relay(7)
        finish_proj(0, True)
        far_w(4)
        far_w(5)
        for k in range(4):
            project(k, 1, 4, 6, False)
        finish_proj(0, False)
        send_state(0)
        o_relay(sl_out, (early, early + 1), True, False)
        far_w(6)
        o_relay(sl_out, (early + 2,), True, False)
        far_w(7)
        for k in (2, 0):
            project(k, 1, 6, w_pieces, False)
            send_part(k, 1)
        for c in range(early, min(early + 3, out_pieces - whole_pieces)):
            across(sl_out, c).start()
        for k in (1, 3):
            project(k, 1, 6, w_pieces, False)
            send_qk(k, 1)
        o_relay(sl_out, range(early + 3, out_pieces), True)
        attend_own(0)
        o_relay(sl_far, (early, early + 1), False)
        attend_prior(0)
        finish_proj(1, False)
        o_relay(sl_far, range(early + 2, early + 4), False)
        finish_proj(1, True)
        send_state(1)
        spread_nums(0)
        attend_own(1)

        @pl.when(high)
        def _():
            o_relay(sl_far, range(early + 4, out_pieces), False)

        attend_prior(1)
        spread_nums(1)

        @pl.when(low)
        def _():
            o_relay(sl_far, range(early + 4, out_pieces), False)

        nums_passed(0)
        nums_gathered(0)
        multiply(my, True, first=True)
        multiply(second, False)
        nums_passed(1)
        nums_gathered(1)
        multiply(sl_out, False)
        multiply(sl_far, False, last=True)

    @pl.when(outer)
    def _():
        for r in range(row_chunks):
            tok_arrive(0, quarter, r)
            z_tok(2, r).start()
        for c in range(w_pieces):
            w_loaded(c)
            w_copy(my, c).start()
        for c in late:
            o_copy(my, c, True, True).start()
        for c in range(out_pieces - whole_pieces, out_pieces):
            o_other(c).start()
        o_relay(near, range(out_pieces), None)
        o_relay(second, range(out_pieces), None)
        o_relay(sl_far, range(early), None)
        nums_taken(0)
        o_relay(sl_far, range(early, early + 2), None)

        @pl.when(high)
        def _():
            o_relay(sl_far, range(early + 2, early + 4), None)

        nums_passed(0)

        @pl.when(low)
        def _():
            o_relay(sl_far, range(early + 2, early + 4), None)
            nums_taken(1)

        @pl.when(high)
        def _():
            o_relay(sl_far, range(early + 4, out_pieces), None)

        nums_gathered(0)
        multiply(near, False, first=True)

        @pl.when(low)
        def _():
            o_relay(sl_far, range(early + 4, out_pieces), None)

        multiply(second, False)

        @pl.when(high)
        def _():
            nums_taken(1)

        nums_passed(1)
        nums_gathered(1)
        multiply(my, True)
        multiply(sl_far, False, last=True)

    def flush(whole, sem):
        remote(whole, whole, sem, sem, {"sub": 1 - s}).wait_send()

    def tok_flush(k, kind):
        flush(xq.at[k, quarter], tok_s.at[k, kind])

    for role, gate in (("inner", inner), ("outer", outer), ("low", inner & low)):

        @pl.when(gate)
        def _():
            for make, args in logs[role]:
                make(*args).wait_send()

    @pl.when(inner)
    def _():
        for h in (my, sl_out):
            flush(wall.at[:, h], w_ss.at[h])
            flush(wobuf.at[h, g], o_in.at[h])
        for h in (my, second, sl_far):
            flush(wobuf.at[h, g], o_out.at[h])
        for h in (second, sl_far):
            flush(wobuf.at[h, g], o_ac.at[h])
        flush(wobuf.at[sl_out, g, pl.ds(0, out_pieces - whole_pieces)], o_ac.at[sl_out])
        for k in range(3):
            for kind in (1, 2, 3):
                tok_flush(k, kind)

    @pl.when(outer)
    def _():
        flush(wall.at[:, my], w_ss.at[my])
        flush(wobuf.at[my, g], o_in.at[my])
        for h in (near, second, sl_far):
            flush(wobuf.at[h, g], o_ac.at[h])
        flush(wobuf.at[my, g, pl.ds(0, whole_pieces)], o_ac.at[my])
        for k in (1, 2):
            tok_flush(k, 0)

    tok_flush(0, 0)
    for stack in range(2):
        for kind in range(3):
            spread_num(stack, kind).wait_send()
    for r in range(row_chunks):
        out_copy(r).wait()


def per_device_line(n, tokens, norm_gain, w_query, w_key, w_value, head_gain, w_out):
    count, width = tokens.shape
    shards = [w_query[0], w_key[0], w_value[0]]
    rows = sum(shard.shape[0] for shard in shards)
    qk_rows = w_query.shape[1] + w_key.shape[1]
    channels = w_value.shape[1]
    head_width, columns = w_out.shape[1], w_out.shape[2]
    pieces, w_pieces, out_pieces, row_chunks = 4, 8, 8, 4
    early, whole_pieces, direct = 3, 3, 2
    span = width // (2 * pieces)
    products = qk_rows * qk_rows * 3 // 4 + qk_rows + 1
    feature_rows = -(-products // 128) * 128
    wo = w_out.reshape(2, out_pieces, head_width // out_pieces, columns)
    hbm = pl.BlockSpec(memory_space=pl.ANY)
    vmem = pl.BlockSpec(memory_space=pltpu.VMEM)
    dma = pltpu.SemaphoreType.DMA
    return pl.pallas_call(
        functools.partial(line_kernel, n, pieces, w_pieces, out_pieces, early, whole_pieces, direct, row_chunks),
        out_shape=jax.ShapeDtypeStruct((count, columns), BF16),
        in_specs=[hbm, vmem, vmem, hbm] + [hbm] * 3,
        out_specs=hbm,
        scratch_shapes=[
            pltpu.VMEM(tokens.shape, BF16),
            pltpu.VMEM(wo.shape, BF16),
            pltpu.VMEM((count, columns), BF16),
            dma((w_pieces + 1 + row_chunks,)),
            dma((row_chunks,)),
            pltpu.VMEM((count, span), BF16),
            pltpu.VMEM((count, span), BF16),
            pltpu.VMEM((pieces, count, span), BF16),
            pltpu.VMEM((3, pieces, count, span), BF16),
            pltpu.VMEM((w_pieces, n, rows, span * pieces // w_pieces), BF16),
            pltpu.VMEM((n,) + wo.shape, BF16),
            pltpu.VMEM((4, n // 2, 2 * rows, count), F32),
            pltpu.VMEM((2, n, rows, count), BF16),
            pltpu.VMEM((2, n, rows, count), BF16),
            pltpu.VMEM((2, 2, n, qk_rows, count), BF16),
            pltpu.VMEM((n, qk_rows, 2 * count), BF16),
            pltpu.VMEM((n, rows, 2 * count), BF16),
            pltpu.VMEM((n, channels, feature_rows), BF16),
            pltpu.VMEM((n, channels, feature_rows), BF16),
            pltpu.VMEM((2, feature_rows, 2 * count), BF16),
            pltpu.VMEM((2, n, qk_rows, count), BF16),
            pltpu.VMEM((2, channels, 2 * count), F32),
            pltpu.VMEM((n, channels, count), BF16),
            pltpu.VMEM((n, 2, 2, channels, count), BF16),
            pltpu.VMEM((n, count, 2 * head_width), BF16),
            pltpu.VMEM((count, columns), F32),
            dma((n,)),
            dma((n, w_pieces)),
            dma((3, 4)),
            dma((3, pieces, row_chunks)),
            dma((n,)),
            dma((n,)),
            dma((n, out_pieces)),
            dma((n,)),
            dma((n,)),
            dma((2, n // 2)),
            dma((2, n // 2)),
            dma((2, n // 2, 2)),
            dma((2, n // 2, 2)),
            dma((n // 2,)),
            dma((n // 2,)),
            dma((n // 2,)),
            dma((n // 2, 3)),
            dma((n // 2, 2, 2)),
            pltpu.SemaphoreType.REGULAR,
        ],
        compiler_params=pltpu.CompilerParams(
            collective_id=0, has_side_effects=True, vmem_limit_bytes=60 * 1024 * 1024
        ),
    )(tokens, norm_gain.reshape(1, -1), head_gain.reshape(1, -1), wo, *shards)


def per_device(sizes, tokens, norm_gain, w_query, w_key, w_value, head_gain, w_out):
    n, nf, ns = sizes
    shards = [w_query[0], w_key[0], w_value[0]]
    if any(shard.shape[0] % 8 for shard in shards):
        shards = [jnp.concatenate(shards, 0)]
    rows, width = sum(shard.shape[0] for shard in shards), tokens.shape[1]
    count = tokens.shape[0]
    qk_rows = w_query.shape[1] + w_key.shape[1]
    channels = w_value.shape[1]
    head_width, columns = w_out.shape[1], w_out.shape[2]
    pieces = max(1, 16 // n)
    out_pieces = max(1, 16 // n)
    wo = w_out.reshape(ns, out_pieces, head_width // out_pieces, columns)
    hbm = pl.BlockSpec(memory_space=pl.ANY)
    vmem = pl.BlockSpec(memory_space=pltpu.VMEM)
    dma = pltpu.SemaphoreType.DMA
    return pl.pallas_call(
        functools.partial(kernel, n, nf, ns, pieces, out_pieces, len(shards)),
        out_shape=jax.ShapeDtypeStruct((count, columns), BF16),
        in_specs=[hbm, vmem, vmem, hbm] + [hbm] * len(shards),
        out_specs=vmem,
        scratch_shapes=[
            pltpu.VMEM(tokens.shape, BF16),
            pltpu.VMEM((rows, width), BF16),
            pltpu.VMEM(wo.shape, BF16),
            dma((len(shards) + 2,)),
            pltpu.VMEM((2 * pieces, count, width // (2 * pieces)), BF16),
            pltpu.VMEM((n, 2, pieces, rows, width // (2 * pieces)), BF16),
            pltpu.VMEM((n,) + wo.shape, BF16),
            pltpu.VMEM((n, qk_rows, count), BF16),
            pltpu.VMEM((n, channels, count), BF16),
            pltpu.VMEM((n, nf, qk_rows, count), BF16),
            pltpu.VMEM((n, channels, count), BF16),
            pltpu.VMEM((n, nf * qk_rows // 2, count), BF16),
            pltpu.VMEM((n, nf * qk_rows // 2, count), BF16),
            pltpu.VMEM((n, channels, count), BF16),
            pltpu.VMEM((n, nf, ns, channels, count), BF16),
            pltpu.VMEM((n, count, ns * head_width), BF16),
            pltpu.VMEM((count, columns), F32),
        ]
        + [dma((n, pieces))] * 5
        + [dma((n, out_pieces))] * 5
        + [
            dma((n, nf)),
            dma((n, nf)),
            dma((n,)),
            dma((n,)),
            dma((n,)),
            dma((n,)),
            dma((n, nf, ns)),
            dma((n, nf, ns)),
        ],
        compiler_params=pltpu.CompilerParams(
            collective_id=0, has_side_effects=True, vmem_limit_bytes=60 * 1024 * 1024
        ),
    )(tokens, norm_gain.reshape(1, -1), head_gain.reshape(1, -1), wo, *shards)


def solution(mesh):
    in_specs = (
        P(("groups", "seq"), None),
        P(),
        P(("seq", "sub"), "fsdp", None),
        P(("seq", "sub"), "fsdp", None),
        P(("seq", "sub"), "fsdp", None),
        P(),
        P("seq", None, ("fsdp", "sub")),
    )
    out_specs = P(("groups", "seq"), ("fsdp", "sub"))
    sizes = (mesh.shape["seq"], mesh.shape["fsdp"], mesh.shape["sub"])
    if sizes == (4, 2, 2):
        body = functools.partial(per_device_line, sizes[0])
    else:
        body = functools.partial(per_device, sizes)
    return jax.shard_map(
        body,
        mesh=mesh,
        in_specs=in_specs,
        out_specs=out_specs,
        check_vma=False,
    )
```

```python
import functools

import jax
import jax.numpy as jnp
from jax import lax
from jax.experimental import pallas as pl
from jax.experimental.pallas import tpu as pltpu
from jax.sharding import PartitionSpec as P

MESH = pl.DeviceIdType.MESH
F32 = jnp.float32
BF16 = jnp.bfloat16


def kernel(
    n,
    nf,
    ns,
    pieces,
    out_pieces,
    w_count,
    tok_hbm,
    gain_ref,
    head_gain_ref,
    wo_hbm,
    *rest,
):
    kernel_body(
        n, nf, ns, pieces, out_pieces, tok_hbm, gain_ref, head_gain_ref, wo_hbm,
        rest[:w_count], *rest[w_count:]
    )


def kernel_body(
    n,
    nf,
    ns,
    pieces,
    out_pieces,
    tok_hbm,
    gain_ref,
    head_gain_ref,
    wo_hbm,
    w_hbm,
    out_ref,
    tok_ref,
    w_ref,
    wo_ref,
    load_sem,
    normed,
    wbuf,
    wobuf,
    qk_send,
    v_send,
    qk_all,
    v_all,
    q_full,
    k_full,
    num_send,
    num_all,
    attended,
    total,
    w_zrecv,
    w_yrecv,
    w_right,
    w_left,
    w_across,
    o_zrecv,
    o_yrecv,
    o_right,
    o_left,
    o_across,
    qk_ssem,
    qk_rsem,
    v_ssem,
    v_rsem,
    num_ssem,
    num_rsem,
    sib_ssem,
    sib_rsem,
):
    group = lax.axis_index("groups")
    me = lax.axis_index("seq")
    my_f = lax.axis_index("fsdp")
    my_s = lax.axis_index("sub")
    tokens, width = tok_ref.shape

    loads = []
    row = 0
    for k, source in enumerate(w_hbm):
        size = source.shape[0]
        target = w_ref.at[pl.ds(row, size)] if len(w_hbm) > 1 else w_ref
        loads.append(pltpu.make_async_copy(source, target, load_sem.at[k]))
        row += size
    tok_load = pltpu.make_async_copy(tok_hbm, tok_ref, load_sem.at[len(w_hbm)])
    wo_load = pltpu.make_async_copy(wo_hbm, wo_ref, load_sem.at[len(w_hbm) + 1])
    for load in loads + [tok_load, wo_load]:
        load.start()

    peers = [
        {"seq": lax.rem(me + dz, n), "fsdp": lax.rem(my_f + df, nf)}
        for dz in range(n)
        for df in range(nf)
        if dz or df
    ]
    peers += [
        {"fsdp": lax.rem(my_f + df, nf), "sub": lax.rem(my_s + ds, ns)}
        for df in range(nf)
        for ds in range(1, ns)
    ]
    peers += [{"groups": 1 - group}]
    barrier = pltpu.get_barrier_semaphore()
    for peer in peers:
        pl.semaphore_signal(barrier, inc=1, device_id=peer, device_id_type=MESH)
    pl.semaphore_wait(barrier, len(peers))
    for load in loads:
        load.wait()
    span = width // (2 * pieces)
    qk_rows = qk_all.shape[2]
    half_rows = qk_rows // 2

    def own_w(c):
        start = pl.multiple_of((group * pieces + c) * span, span)
        return w_ref.at[:, pl.ds(start, span)]

    def own_o(c):
        return wo_ref.at[group, c]

    class Stream:
        def __init__(self, own, buf, count, zrecv, yrecv, right, left, across):
            self.own, self.buf, self.count = own, buf, count
            self.zrecv, self.yrecv = zrecv, yrecv
            self.right_sem, self.left_sem, self.across_sem = right, left, across

        def along(self, o, c, sems, target, own):
            slot = self.buf.at[o, group, c]
            return pltpu.make_async_remote_copy(
                src_ref=self.own(c) if own else slot,
                dst_ref=slot,
                send_sem=sems.at[o, c],
                recv_sem=self.zrecv.at[o, c],
                device_id={"seq": target},
                device_id_type=MESH,
            )

        def right(self, o, c, own=False):
            return self.along(o, c, self.right_sem, me + 1, own)

        def left(self, o, c, own=False):
            return self.along(o, c, self.left_sem, me - 1, own)

        def across(self, o, c, half):
            slot = self.buf.at[o, half, c]
            return pltpu.make_async_remote_copy(
                src_ref=slot,
                dst_ref=slot,
                send_sem=self.across_sem.at[o, c],
                recv_sem=self.yrecv.at[o, c],
                device_id={"groups": 1 - group},
                device_id_type=MESH,
            )

        def begin(self):
            for c in range(self.count):

                @pl.when(me + 1 < n)
                def _():
                    self.right(me, c, True).start()

                @pl.when(me >= 1)
                def _():
                    self.left(me, c, True).start()

        def relay(self, r, between=None):
            for c in range(self.count):
                if between is not None and c == self.count // 2:
                    between()

                @pl.when(me >= r)
                def _():
                    o = me - r
                    self.right(o, c).wait_recv()

                    @pl.when(me + 1 < n)
                    def _():
                        self.right(o, c).start()

                    self.across(o, c, group).start()

                @pl.when(me + r < n)
                def _():
                    o = me + r
                    self.left(o, c).wait_recv()

                    @pl.when(me >= 1)
                    def _():
                        self.left(o, c).start()

                    self.across(o, c, group).start()

        def arrive(self, o):
            for c in range(self.count):
                self.across(o, c, 1 - group).wait_recv()

        def finish(self):
            for r in range(n):
                for c in range(self.count):

                    @pl.when((me >= r) & (me + 1 < n))
                    def _():
                        self.right(me - r, c, r == 0).wait_send()

                    @pl.when((me + r < n) & (me >= 1))
                    def _():
                        self.left(me + r, c, r == 0).wait_send()

                    if r > 0:

                        @pl.when(me >= r)
                        def _():
                            self.across(me - r, c, group).wait_send()

                        @pl.when(me + r < n)
                        def _():
                            self.across(me + r, c, group).wait_send()

    w_stream = Stream(own_w, wbuf, pieces, w_zrecv, w_yrecv, w_right, w_left, w_across)
    o_stream = Stream(own_o, wobuf, out_pieces, o_zrecv, o_yrecv, o_right, o_left, o_across)

    w_stream.begin()
    wo_load.wait()
    at_end = (me == 0) | (me == n - 1)

    @pl.when(at_end)
    def _():
        o_stream.begin()

    tok_load.wait()

    row_step = 16

    def norm_rows(i, carry):
        rows = pl.ds(pl.multiple_of(i * row_step, row_step), row_step)
        sumsq = jnp.zeros((row_step, 1), F32)
        for c in range(2 * pieces):
            part = tok_ref[rows, c * span : (c + 1) * span].astype(F32)
            sumsq = sumsq + jnp.sum(part * part, axis=1, keepdims=True)
        scale = lax.rsqrt(sumsq / width + 1e-05)
        for c in range(2 * pieces):
            cols = slice(c * span, (c + 1) * span)
            part = tok_ref[rows, cols].astype(F32)
            normed[c, rows, :] = (part * scale * gain_ref[:, cols]).astype(BF16)
        return carry

    lax.fori_loop(0, tokens // row_step, norm_rows, 0)

    def contract(weights, acts):
        return lax.dot_general(weights, acts, (((1,), (1,)), ((), ())), preferred_element_type=F32)

    def qk_copy(o, source, other_f, token_block, f_from):
        return pltpu.make_async_remote_copy(
            src_ref=source,
            dst_ref=qk_all.at[token_block, f_from],
            send_sem=qk_ssem.at[o, other_f],
            recv_sem=qk_rsem.at[token_block, f_from],
            device_id={"seq": o, "fsdp": other_f},
            device_id_type=MESH,
        )

    def v_copy(o, token_block):
        return pltpu.make_async_remote_copy(
            src_ref=v_send.at[o],
            dst_ref=v_all.at[token_block],
            send_sem=v_ssem.at[o],
            recv_sem=v_rsem.at[token_block],
            device_id={"seq": o},
            device_id_type=MESH,
        )

    def project_own():
        acc = jnp.zeros((w_ref.shape[0], tokens), F32)
        for c in range(2 * pieces):
            acc = acc + contract(w_ref[:, c * span : (c + 1) * span], normed[c])
        qk_all[me, my_f] = acc[:qk_rows].astype(BF16)
        v_all[me] = acc[qk_rows:].astype(BF16)
        for df in range(1, nf):
            other = lax.rem(my_f + df, nf)
            qk_copy(me, qk_all.at[me, my_f], other, me, my_f).start()

    def project(o):
        def body(c, acc):
            return acc + contract(wbuf[o, c // pieces, c % pieces], normed[c])

        acc = lax.fori_loop(0, 2 * pieces, body, jnp.zeros((w_ref.shape[0], tokens), F32))
        qk_send[o] = acc[:qk_rows].astype(BF16)
        v_send[o] = acc[qk_rows:].astype(BF16)
        for df in range(nf):
            qk_copy(o, qk_send.at[o], lax.rem(my_f + df, nf), me, my_f).start()
        v_copy(o, me).start()

    def both(r, action):
        @pl.when(me >= r)
        def _():
            action(me - r)

        @pl.when(me + r < n)
        def _():
            action(me + r)

    def take(o):
        w_stream.arrive(o)
        project(o)

    project_own()
    for r in range(1, n):
        if r == n - 1:

            @pl.when(jnp.logical_not(at_end))
            def _():
                o_stream.begin()

        w_stream.relay(r, functools.partial(both, r - 1, take) if r > 1 else None)

    o_stream.relay(1, functools.partial(both, n - 1, take))

    def gather_heads():
        for d in range(1, n):
            t = lax.rem(me + d, n)
            v_copy(me, t).wait_recv()
            for df in range(nf):
                qk_copy(me, qk_all.at[t, df], 0, t, df).wait_recv()
        for df in range(1, nf):
            other = lax.rem(my_f + df, nf)
            qk_copy(me, qk_all.at[me, other], other, me, other).wait_recv()

        for t in range(n):
            parts = [qk_all[t, f].astype(F32) for f in range(nf)]
            q_full[t] = jnp.concatenate([p[:half_rows] for p in parts], 0).astype(BF16)
            k_full[t] = jnp.concatenate([p[half_rows:] for p in parts], 0).astype(BF16)

    channels = v_all.shape[1]
    key_pos = lax.broadcasted_iota(jnp.int32, (tokens, tokens), 0)
    query_pos = lax.broadcasted_iota(jnp.int32, (tokens, tokens), 1)

    def numerator(t):
        queries = q_full[t]

        def body(j, acc):
            scores = lax.dot_general(
                k_full[j], queries, (((0,), (0,)), ((), ())), preferred_element_type=F32
            )
            value = 1.0 + scores * 0.25 + scores * scores * 0.03125
            weight = jnp.where(key_pos + (j - t) * tokens <= query_pos, value, 0.0).astype(BF16)
            return acc + jnp.dot(v_all[j], weight, preferred_element_type=F32)

        acc = lax.fori_loop(0, t + 1, body, jnp.zeros((channels, tokens), F32))
        return acc.astype(BF16)

    def num_copy(t, head_block):
        return pltpu.make_async_remote_copy(
            src_ref=num_send.at[t],
            dst_ref=num_all.at[head_block, my_f, my_s],
            send_sem=num_ssem.at[t],
            recv_sem=num_rsem.at[head_block],
            device_id={"seq": t},
            device_id_type=MESH,
        )

    def sib_copy(o, to_f, to_s, from_f, from_s):
        slot = num_all.at[o, from_f, from_s]
        return pltpu.make_async_remote_copy(
            src_ref=slot,
            dst_ref=slot,
            send_sem=sib_ssem.at[o, to_f, to_s],
            recv_sem=sib_rsem.at[o, from_f, from_s],
            device_id={"fsdp": to_f, "sub": to_s},
            device_id_type=MESH,
        )

    def siblings():
        for df in range(nf):
            for ds in range(ns):
                if df or ds:
                    yield lax.rem(my_f + df, nf), lax.rem(my_s + ds, ns)

    def attend():
        gather_heads()
        for d in range(1, n):
            t = lax.rem(me + d, n)
            num_send[t] = numerator(t)
            num_copy(t, me).start()
        num_all[me, my_f, my_s] = numerator(me)
        for f, s in siblings():
            sib_copy(me, f, s, my_f, my_s).start()

    def spread():
        for d in range(1, n):
            o = lax.rem(me + d, n)
            num_copy(o, o).wait_recv()
            for f, s in siblings():
                sib_copy(o, f, s, my_f, my_s).start()

    for r in range(2, n):
        o_stream.relay(r, {2: attend, 3: spread}.get(r))

    for d in range(n):
        o = lax.rem(me + d, n)
        for f, s in siblings():
            sib_copy(o, f, s, f, s).wait_recv()

    head_width = nf * channels

    def attend_block(o, carry):
        for s in range(ns):
            whole = jnp.concatenate([num_all[o, f, s] for f in range(nf)], 0).astype(F32)
            meansq = jnp.sum(whole * whole, axis=0, keepdims=True) / head_width
            scaled = (whole * lax.rsqrt(meansq + 1e-06)).T * head_gain_ref[...]
            attended[o, :, s * head_width : (s + 1) * head_width] = scaled.astype(BF16)
        return carry

    lax.fori_loop(0, n, attend_block, 0)

    columns = out_ref.shape[1]
    depth = ns * head_width

    total[...] = jnp.dot(
        attended[me], wo_ref[...].reshape(depth, columns), preferred_element_type=F32
    )

    def multiply(o):
        o_stream.arrive(o)
        total[...] += jnp.dot(
            attended[o], wobuf[o].reshape(depth, columns), preferred_element_type=F32
        )

    for r in range(1, n):
        both(r, multiply)
    out_ref[...] = total[...].astype(BF16)

    w_stream.finish()
    o_stream.finish()
    for d in range(n):
        o = lax.rem(me + d, n)
        for df in range(nf):
            if d or df:
                other = lax.rem(my_f + df, nf)
                source = qk_send.at[o] if d else qk_all.at[me, my_f]
                qk_copy(o, source, other, me, my_f).wait_send()
        if d:
            v_copy(o, me).wait_send()
            num_copy(o, me).wait_send()
        for f, s in siblings():
            sib_copy(o, f, s, my_f, my_s).wait_send()

def line_kernel(
    n,
    pieces,
    w_pieces,
    out_pieces,
    early,
    whole_pieces,
    direct,
    row_chunks,
    tok_hbm,
    gain_ref,
    head_gain_ref,
    wo_hbm,
    wq_hbm,
    wk_hbm,
    wv_hbm,
    out_hbm,
    tok_ref,
    wo_ref,
    out_ref,
    load_sem,
    out_sem,
    ysend,
    ysend2,
    xn,
    xq,
    wall,
    wobuf,
    acc,
    part_send,
    part_recv,
    qk,
    q_full,
    kv,
    state,
    state_in,
    feats,
    qk_mine,
    nacc,
    num_send,
    num_all,
    attended,
    total,
    w_ss,
    w_rs,
    tok_s,
    tok_r,
    tok_x,
    tok_w,
    o_out,
    o_in,
    o_rs,
    o_ac,
    o_yr,
    part_s,
    part_r,
    qk_s,
    qk_r,
    kv_s,
    kv_r,
    num_s,
    ng_s,
    ng_r,
    beyond,
):
    g = lax.axis_index("groups")
    z = lax.axis_index("seq")
    f = lax.axis_index("fsdp")
    s = lax.axis_index("sub")
    upper = z // (n // 2)
    sign = 2 * upper - 1
    out_z = z + sign
    in_z = z - sign
    inner = (z > 0) & (z < n - 1)
    outer = jnp.logical_not(inner)
    low = upper == 0
    high = upper == 1
    near = upper
    second = 1 - upper
    ends = n - 2
    my = jnp.where(inner, upper, ends + upper)
    sl_out = ends + upper
    sl_far = ends + 1 - upper
    p_own = 1 - upper
    p_end = upper
    tokens, width = tok_ref.shape
    rows, w_span = wall.shape[2], wall.shape[3]
    span = xn.shape[2]
    split = span // w_span
    qk_rows = qk.shape[3]
    half_rows = qk_rows // 2
    quarter = f * 2 + s
    f_other = 1 - f
    q_sib = f * 2 + 1 - s
    q_x = (1 - f) * 2 + s
    q_diag = (1 - f) * 2 + 1 - s

    loads = []
    for c in range(w_pieces):
        row = 0
        for source in (wq_hbm, wk_hbm, wv_hbm):
            size = source.shape[0]
            col = pl.multiple_of((g * w_pieces + c) * w_span, w_span)
            loads.append(
                pltpu.make_async_copy(
                    source.at[:, pl.ds(col, w_span)],
                    wall.at[c, my, pl.ds(row, size)],
                    load_sem.at[c],
                )
            )
            row += size

    def w_loaded(c):
        slot = wall.at[c, my]
        pltpu.make_async_copy(slot, slot, load_sem.at[c]).wait()

    wo_load = pltpu.make_async_copy(wo_hbm, wo_ref, load_sem.at[w_pieces])
    step = tokens // row_chunks
    tok_loads = [
        pltpu.make_async_copy(
            tok_hbm.at[pl.ds(r * step, step)],
            tok_ref.at[pl.ds(r * step, step)],
            load_sem.at[w_pieces + 1 + r],
        )
        for r in range(row_chunks)
    ]

    @pl.when(inner)
    def _():
        for load in loads + tok_loads + [wo_load]:
            load.start()

    @pl.when(outer)
    def _():
        for load in [wo_load] + tok_loads + loads:
            load.start()

    barrier = pltpu.get_barrier_semaphore()
    for peer in (
        {"seq": in_z},
        {"groups": 1 - g},
        {"fsdp": 1 - f},
        {"sub": 1 - s},
    ):
        pl.semaphore_signal(barrier, inc=1, device_id=peer, device_id_type=MESH)

    @pl.when(inner)
    def _():
        pl.semaphore_signal(barrier, inc=1, device_id={"seq": out_z}, device_id_type=MESH)
        pl.semaphore_wait(barrier, 5)
        pl.semaphore_signal(beyond, inc=1, device_id={"fsdp": 1 - f}, device_id_type=MESH)

    @pl.when(outer)
    def _():
        pl.semaphore_wait(barrier, 4)

    logs = {"inner": [], "outer": [], "all": [], "low": []}

    def launch(role, make, *args):
        make(*args).start()
        logs[role].append((make, args))

    def remote(src, dst, send, recv, to):
        return pltpu.make_async_remote_copy(
            src_ref=src,
            dst_ref=dst,
            send_sem=send,
            recv_sem=recv,
            device_id=to,
            device_id_type=MESH,
        )

    def w_copy(h, c):
        slot = wall.at[c, h]
        return remote(slot, slot, w_ss.at[h], w_rs.at[h, c], {"seq": in_z})

    def o_copy(h, c, own, inward):
        slot = wobuf.at[h, g, c]
        return remote(
            wo_ref.at[g, c] if own else slot,
            slot,
            (o_in if inward else o_out).at[h],
            o_rs.at[h, c],
            {"seq": in_z if inward else out_z},
        )

    def o_other(c):
        return remote(
            wo_ref.at[1 - g, c], wobuf.at[my, 1 - g, c], o_ac.at[my], o_yr.at[my], {"seq": in_z}
        )

    def across(h, c):
        slot = wobuf.at[h, g, c]
        return remote(slot, slot, o_ac.at[h], o_yr.at[h], {"groups": 1 - g})

    def crossed(h):
        slot = wobuf.at[h, 1 - g]
        remote(slot, slot, o_ac.at[h], o_yr.at[h], {"groups": 1 - g}).wait_recv()

    def part_rows(r):
        return pl.ds(r * step, step)

    def y_tok(r):
        return remote(
            ysend.at[part_rows(r)],
            xq.at[0, quarter, part_rows(r)],
            tok_s.at[0, 0],
            tok_r.at[0, r],
            {"groups": 1 - g},
        )

    def y_tok2(r):
        return remote(
            ysend2.at[part_rows(r)],
            xq.at[0, q_x, part_rows(r)],
            tok_s.at[0, 2],
            tok_x.at[0, r],
            {"groups": 1 - g},
        )

    def z_tok(k, r):
        src = xn.at[quarter, part_rows(r)] if k == 1 else xq.at[0, quarter, part_rows(r)]
        return remote(
            src,
            xq.at[k, quarter, part_rows(r)],
            tok_s.at[k, 0],
            tok_r.at[k, r],
            {"seq": in_z},
        )

    def spread_tok(k, c, r, kind):
        slot = xq.at[k, c, part_rows(r)]
        to = {"fsdp": 1 - f} if kind == 2 else {"sub": 1 - s}
        sem = tok_x.at[k, r] if kind == 2 else tok_w.at[k, kind // 2]
        return remote(slot, slot, tok_s.at[k, kind], sem, to)

    def tok_arrive(k, r):
        slot = xq.at[k, quarter, part_rows(r)]
        remote(slot, slot, tok_s.at[k, 1], tok_r.at[k, r], {"sub": 1 - s}).wait_recv()

    def gather_own(k, r):
        tok_arrive(k, r)
        if k > 0 or r < direct:
            spread_tok(k, quarter, r, 2).start()
        spread_tok(k, quarter, r, 1).start()

    def gather_fwd(k, r):
        slot = xq.at[k, q_x, part_rows(r)]
        remote(slot, slot, tok_s.at[k, 1], tok_x.at[k, r], {"sub": 1 - s}).wait_recv()
        spread_tok(k, q_x, r, 3).start()

    def gathered(k):
        for i, c in enumerate((q_sib, q_diag)):
            slot = xq.at[k, c]
            remote(slot, slot, tok_s.at[k, 1], tok_w.at[k, i], {"sub": 1 - s}).wait_recv()

    def both(stack):
        return pl.ds(2 * stack, 2)

    def part_copy(p, stack):
        return remote(
            part_send.at[p, both(stack)],
            part_recv.at[p, both(stack)],
            part_s.at[p, stack],
            part_r.at[p, stack],
            {"groups": 1 - g},
        )

    def qk_copy(p, stack, way):
        if way:
            src = part_send.at[p, both(stack), pl.ds(0, qk_rows)]
            to = {"groups": 1 - g, "fsdp": 1 - f}
        else:
            src, to = qk_mine.at[p, both(stack)], {"fsdp": 1 - f}
        return remote(
            src, qk.at[p, way, both(stack)], qk_s.at[p, stack, way], qk_r.at[p, stack, way], to
        )

    def lanes(p):
        start = p * tokens
        return pl.ds(start if isinstance(p, int) else pl.multiple_of(start, tokens), tokens)

    def state_copy(stack):
        return remote(
            state.at[both(stack)],
            state_in.at[both(stack)],
            kv_s.at[stack],
            kv_r.at[stack],
            {"seq": in_z},
        )

    def num_copy(stack):
        return remote(
            num_send.at[both(stack)],
            num_all.at[both(stack), f, s],
            num_s.at[stack],
            ng_r.at[stack, f, s],
            {"seq": out_z},
        )

    def spread_num(stack, kind):
        ff = f_other if kind == 2 else f
        slot = num_all.at[both(stack), ff, s]
        to = {"fsdp": 1 - f} if kind == 1 else {"sub": 1 - s}
        return remote(slot, slot, ng_s.at[stack, kind], ng_r.at[stack, ff, s], to)

    def num_arrive(stack, ff, ss):
        slot = num_all.at[both(stack), ff, ss]
        remote(slot, slot, ng_s.at[stack, 0], ng_r.at[stack, ff, ss], {"sub": 1 - s}).wait_recv()

    def nums_taken(stack):
        num_arrive(stack, f, s)
        for kind in (1, 0):
            spread_num(stack, kind).start()

    def nums_passed(stack):
        num_arrive(stack, 1 - f, s)
        spread_num(stack, 2).start()

    def nums_gathered(stack):
        num_arrive(stack, f, 1 - s)
        num_arrive(stack, 1 - f, 1 - s)

    @pl.when(inner)
    def _():
        for c in range(w_pieces):
            w_loaded(c)
            w_copy(my, c).start()
        wo_load.wait()
        for c in range(out_pieces):
            o_copy(my, c, True, False).start()

    @pl.when(outer)
    def _():
        wo_load.wait()
        for c in range(early):
            o_copy(my, c, True, True).start()

    row_step = 16

    def norm_rows(i, carry):
        block = pl.ds(pl.multiple_of(i * row_step, row_step), row_step)
        sumsq = jnp.zeros((row_step, 1), F32)
        for c in range(2 * pieces):
            part = tok_ref[block, c * span : (c + 1) * span].astype(F32)
            sumsq = sumsq + jnp.sum(part * part, axis=1, keepdims=True)
        scale = lax.rsqrt(sumsq / width + 1e-05)

        def column(c):
            cols = pl.ds(pl.multiple_of(c * span, span), span)
            part = tok_ref[block, cols].astype(F32)
            return (part * scale * gain_ref[:, cols]).astype(BF16)

        ysend[block, :] = column((1 - g) * pieces + quarter)
        ysend2[block, :] = column((1 - g) * pieces + q_x)
        for c in range(pieces):
            xn[c, block, :] = column(g * pieces + c)
        return carry

    per_chunk = step // row_step
    for r in range(row_chunks):
        tok_loads[r].wait()
        lax.fori_loop(r * per_chunk, (r + 1) * per_chunk, norm_rows, 0)
        y_tok(r).start()

        @pl.when(outer)
        def _():
            z_tok(1, r).start()

    @pl.when(inner)
    def _():
        for r in range(direct, row_chunks):
            y_tok2(r).start()

    def contract(weights, acts):
        return lax.dot_general(weights, acts, (((1,), (1,)), ((), ())), preferred_element_type=F32)

    def project(k, stack, lo, hi, fresh):
        if fresh:
            acc[k, stack] = jnp.zeros(acc.shape[2:], F32)

        def dot(j, i):
            weights = wall[j * split + i, 2 * stack : 2 * stack + 2].reshape(2 * rows, w_span)
            where = pl.ds(i * w_span, w_span)
            return contract(weights, xn[j, :, where] if k == 3 else xq[k, j, :, where])

        def body(j, carry):
            acc[k, stack] += sum([dot(j, i) for i in range(1, split)], dot(j, 0))
            return carry

        lax.fori_loop(lo // split, hi // split, body, 0)

    def send_part(k, stack):
        p = p_own if k == 0 else p_end
        for i in range(2):
            part_send[p, 2 * stack + i] = acc[k, stack, i * rows : (i + 1) * rows].astype(BF16)
        launch("inner", qk_copy, p, stack, 1)
        launch("inner", part_copy, p, stack)

    def send_qk(k, stack):
        p = p_own if k == 3 else p_end
        for i in range(2):
            part = acc[k, stack, i * rows : i * rows + qk_rows]
            qk_mine[p, 2 * stack + i] = part.astype(BF16)
        launch("inner", qk_copy, p, stack, 0)

    def finish_proj(stack, own):
        p, k = (p_own, 3) if own else (p_end, 1)
        part_copy(p, stack).wait_recv()
        for way in range(2):
            qk_copy(p, stack, way).wait_recv()
        for i in range(2):
            h = 2 * stack + i
            whole = acc[k, stack, i * rows : (i + 1) * rows] + part_recv[p, h].astype(F32)
            mine = whole[:qk_rows].astype(BF16).astype(F32)
            other = qk[p, 0, h].astype(F32) + qk[p, 1, h].astype(F32)
            lower = jnp.where(f == 0, mine, other)
            higher = jnp.where(f == 0, other, mine)

            def joined(first):
                last = first + half_rows
                return jnp.concatenate([lower[first:last], higher[first:last]], 0).astype(BF16)

            q_full[h, pl.ds(0, qk_rows), lanes(p)] = joined(0)
            kv[h, pl.ds(0, qk_rows), lanes(p)] = joined(half_rows)
            kv[h, pl.ds(qk_rows, rows - qk_rows), lanes(p)] = whole[qk_rows:].astype(BF16)

    def attend_to(source, queries, causal):
        scores = lax.dot_general(
            source[:qk_rows], queries, (((0,), (0,)), ((), ())), preferred_element_type=F32
        )
        value = 1.0 + scores * 0.25 + scores * scores * 0.03125
        if causal:
            key_pos = lax.broadcasted_iota(jnp.int32, value.shape, 0)
            query_pos = lax.broadcasted_iota(jnp.int32, value.shape, 1)
            value = jnp.where(key_pos <= query_pos, value, 0.0)
        return jnp.dot(source[qk_rows:], value.astype(BF16), preferred_element_type=F32)

    dims = qk_rows
    sub = dims // 2
    used = sub * dims + sub * sub + dims

    def features(vectors):
        x = vectors.astype(F32)
        parts = [x * x[i : i + 1] for i in range(sub)]
        parts += [x[sub:] * x[i : i + 1] for i in range(sub, dims)]
        rest = (feats.shape[1] - used, x.shape[1])
        one = lax.broadcasted_iota(jnp.int32, rest, 0) == 0
        return jnp.concatenate(parts + [x, jnp.where(one, 1.0, 0.0)], 0).astype(BF16)

    def send_state(stack):
        @pl.when(low)
        def _():
            col = lax.broadcasted_iota(jnp.int32, (1, state.shape[2]), 1)
            twice = (col < sub * dims) & (col % dims >= sub)
            factor = jnp.where(twice, 0.0625, 0.03125)
            factor = jnp.where(col >= used - dims, 0.25, factor)
            factor = jnp.where(col >= used, 1.0, factor)
            for h in range(2 * stack, 2 * stack + 2):
                block = kv[h]
                sums = contract(block[qk_rows:], features(block[:qk_rows]))
                state[h] = (sums * factor).astype(BF16)
            launch("low", state_copy, stack)

    def attend_own(stack):
        @pl.when(high)
        def _():
            for i in range(2):
                feats[i] = features(q_full[2 * stack + i])

        for i in range(2):
            h = 2 * stack + i
            nacc[i] = attend_to(kv[h], q_full[h], True)

    def attend_prior(stack):
        @pl.when(high)
        def _():
            state_copy(stack).wait_recv()
            for i in range(2):
                h = 2 * stack + i
                nacc[i] += jnp.dot(state_in[h], feats[i], preferred_element_type=F32)

        for i in range(2):
            num_send[2 * stack + i] = nacc.at[i][:, lanes(p_end)].astype(BF16)
        launch("inner", num_copy, stack)
        for i in range(2):
            num_all[2 * stack + i, f, s] = nacc.at[i][:, lanes(p_own)].astype(BF16)

    def spread_nums(stack):
        for kind in (1, 0):
            spread_num(stack, kind).start()

    def o_relay(h, pieces_now, inward, cross=True):
        for c in pieces_now:
            o_copy(h, c, False, True).wait_recv()
            if inward is not None:
                o_copy(h, c, False, inward).start()
            if cross and not (inward and c >= out_pieces - whole_pieces):
                across(h, c).start()

    def w_relay(c):
        w_copy(sl_out, c).wait_recv()
        w_copy(sl_out, c).start()

    head_width = 2 * num_all.shape[3]
    columns = out_ref.shape[1]
    depth = 2 * head_width

    def attend_block(h):
        for i in range(2):
            whole = jnp.concatenate([num_all[h, j, i] for j in range(2)], 0).astype(F32)
            meansq = jnp.sum(whole * whole, axis=0, keepdims=True) / head_width
            scaled = (whole * lax.rsqrt(meansq + 1e-06)).T * head_gain_ref[...]
            attended[h, :, i * head_width : (i + 1) * head_width] = scaled.astype(BF16)

    out_span = columns // row_chunks

    def out_copy(r):
        block = pl.ds(r * out_span, out_span)
        return pltpu.make_async_copy(out_ref.at[:, block], out_hbm.at[:, block], out_sem.at[r])

    def multiply(h, own, first=False, last=False):
        attend_block(h)
        if not own:
            crossed(h)
        weights = (wo_ref[...] if own else wobuf[h]).reshape(depth, columns)
        if first:
            total[...] = jnp.dot(attended[h], weights, preferred_element_type=F32)
        elif not last:
            total[...] += jnp.dot(attended[h], weights, preferred_element_type=F32)
        else:
            for r in range(row_chunks):
                block = slice(r * out_span, (r + 1) * out_span)
                product = jnp.dot(attended[h], weights[:, block], preferred_element_type=F32)
                out_ref[:, block] = (total[:, block] + product).astype(BF16)
                out_copy(r).start()

    late = range(early, out_pieces)
    def far_w(c):
        w_copy(sl_far, c).wait_recv()

    @pl.when(inner)
    def _():
        for c in range(out_pieces):
            o_copy(my, c, True, True).start()
        o_relay(sl_out, range(early), True)
        gather_own(0, 0)
        gather_own(1, 0)
        gather_own(0, 1)
        gather_fwd(0, 0)
        gather_own(1, 1)
        gather_own(0, 2)
        gather_fwd(1, 0)
        gather_own(1, 2)
        gather_own(0, 3)
        for c in range(w_pieces):
            w_copy(second, c).wait_recv()
        project(3, 0, 0, w_pieces, True)
        send_qk(3, 0)
        gather_fwd(0, 1)
        gather_own(1, 3)
        gather_fwd(0, 2)
        o_relay(second, (0, 1), False)
        gather_fwd(1, 1)
        gather_own(2, 0)
        gather_fwd(0, 3)
        o_relay(second, (2, 3), False)
        gather_fwd(1, 2)
        gather_own(2, 1)
        o_relay(second, (4, 5), False)
        gather_fwd(1, 3)
        gather_own(2, 2)
        gathered(0)
        project(0, 0, 0, w_pieces, True)
        pl.semaphore_wait(beyond, 1)
        send_part(0, 0)
        o_relay(second, (6, 7), False)
        gather_fwd(2, 0)
        gather_own(2, 3)
        gathered(1)
        project(1, 0, 0, w_pieces, True)
        send_qk(1, 0)
        o_relay(sl_far, range(early), False)
        gather_fwd(2, 1)
        w_relay(0)
        w_relay(1)
        gather_fwd(2, 2)
        w_relay(2)
        w_relay(3)
        gather_fwd(2, 3)
        gathered(2)
        project(2, 0, 0, w_pieces, True)
        send_part(2, 0)
        w_relay(4)
        w_relay(5)
        far_w(0)
        far_w(1)
        for k in range(4):
            project(k, 1, 0, 2, True)
        w_relay(6)
        far_w(2)
        far_w(3)
        for k in range(4):
            project(k, 1, 2, 4, False)
        w_relay(7)
        finish_proj(0, True)
        far_w(4)
        far_w(5)
        for k in range(4):
            project(k, 1, 4, 6, False)
        finish_proj(0, False)
        send_state(0)
        o_relay(sl_out, (early, early + 1), True, False)
        far_w(6)
        o_relay(sl_out, (early + 2,), True, False)
        far_w(7)
        for k in (2, 0):
            project(k, 1, 6, w_pieces, False)
            send_part(k, 1)
        for c in range(early, min(early + 3, out_pieces - whole_pieces)):
            across(sl_out, c).start()
        for k in (1, 3):
            project(k, 1, 6, w_pieces, False)
            send_qk(k, 1)
        o_relay(sl_out, range(early + 3, out_pieces), True)
        attend_own(0)
        o_relay(sl_far, (early, early + 1), False)
        attend_prior(0)
        finish_proj(1, False)
        o_relay(sl_far, range(early + 2, early + 4), False)
        finish_proj(1, True)
        send_state(1)
        spread_nums(0)
        attend_own(1)

        @pl.when(high)
        def _():
            o_relay(sl_far, range(early + 4, out_pieces), False)

        attend_prior(1)
        spread_nums(1)

        @pl.when(low)
        def _():
            o_relay(sl_far, range(early + 4, out_pieces), False)

        nums_passed(0)
        nums_gathered(0)
        multiply(my, True, first=True)
        multiply(second, False)
        nums_passed(1)
        nums_gathered(1)
        multiply(sl_out, False)
        multiply(sl_far, False, last=True)

    @pl.when(outer)
    def _():
        for r in range(row_chunks):
            tok_arrive(0, r)
            z_tok(2, r).start()
        for c in range(w_pieces):
            w_loaded(c)
            w_copy(my, c).start()
        for c in late:
            o_copy(my, c, True, True).start()
        for c in range(out_pieces - whole_pieces, out_pieces):
            o_other(c).start()
        o_relay(near, range(out_pieces), None)
        o_relay(second, range(out_pieces), None)
        o_relay(sl_far, range(early), None)
        nums_taken(0)
        o_relay(sl_far, range(early, early + 2), None)

        @pl.when(high)
        def _():
            o_relay(sl_far, range(early + 2, early + 4), None)

        nums_passed(0)

        @pl.when(low)
        def _():
            o_relay(sl_far, range(early + 2, early + 4), None)
            nums_taken(1)

        @pl.when(high)
        def _():
            o_relay(sl_far, range(early + 4, out_pieces), None)

        nums_gathered(0)
        multiply(near, False, first=True)

        @pl.when(low)
        def _():
            o_relay(sl_far, range(early + 4, out_pieces), None)

        multiply(second, False)

        @pl.when(high)
        def _():
            nums_taken(1)

        nums_passed(1)
        nums_gathered(1)
        multiply(my, True)
        multiply(sl_far, False, last=True)

    def flush(whole, sem):
        remote(whole, whole, sem, sem, {"sub": 1 - s}).wait_send()

    def tok_flush(k, kind):
        flush(xq.at[k, quarter], tok_s.at[k, kind])

    for role, gate in (("inner", inner), ("outer", outer), ("low", inner & low)):

        @pl.when(gate)
        def _():
            for make, args in logs[role]:
                make(*args).wait_send()

    @pl.when(inner)
    def _():
        for h in (my, sl_out):
            flush(wall.at[:, h], w_ss.at[h])
            flush(wobuf.at[h, g], o_in.at[h])
        for h in (my, second, sl_far):
            flush(wobuf.at[h, g], o_out.at[h])
        for h in (second, sl_far):
            flush(wobuf.at[h, g], o_ac.at[h])
        flush(wobuf.at[sl_out, g, pl.ds(0, out_pieces - whole_pieces)], o_ac.at[sl_out])
        for k in range(3):
            for kind in (1, 2, 3):
                tok_flush(k, kind)

    @pl.when(outer)
    def _():
        flush(wall.at[:, my], w_ss.at[my])
        flush(wobuf.at[my, g], o_in.at[my])
        for h in (near, second, sl_far):
            flush(wobuf.at[h, g], o_ac.at[h])
        flush(wobuf.at[my, g, pl.ds(0, whole_pieces)], o_ac.at[my])
        for k in (1, 2):
            tok_flush(k, 0)

    tok_flush(0, 0)
    for stack in range(2):
        for kind in range(3):
            spread_num(stack, kind).wait_send()
    for r in range(row_chunks):
        out_copy(r).wait()


def per_device_line(n, tokens, norm_gain, w_query, w_key, w_value, head_gain, w_out):
    count, width = tokens.shape
    shards = [w_query[0], w_key[0], w_value[0]]
    rows = sum(shard.shape[0] for shard in shards)
    qk_rows = w_query.shape[1] + w_key.shape[1]
    channels = w_value.shape[1]
    head_width, columns = w_out.shape[1], w_out.shape[2]
    pieces, w_pieces, out_pieces, row_chunks = 4, 8, 8, 4
    early, whole_pieces, direct = 3, 3, 2
    span = width // (2 * pieces)
    products = qk_rows * qk_rows * 3 // 4 + qk_rows + 1
    feature_rows = -(-products // 128) * 128
    wo = w_out.reshape(2, out_pieces, head_width // out_pieces, columns)
    hbm = pl.BlockSpec(memory_space=pl.ANY)
    vmem = pl.BlockSpec(memory_space=pltpu.VMEM)
    dma = pltpu.SemaphoreType.DMA
    return pl.pallas_call(
        functools.partial(line_kernel, n, pieces, w_pieces, out_pieces, early, whole_pieces, direct, row_chunks),
        out_shape=jax.ShapeDtypeStruct((count, columns), BF16),
        in_specs=[hbm, vmem, vmem, hbm] + [hbm] * 3,
        out_specs=hbm,
        scratch_shapes=[
            pltpu.VMEM(tokens.shape, BF16),
            pltpu.VMEM(wo.shape, BF16),
            pltpu.VMEM((count, columns), BF16),
            dma((w_pieces + 1 + row_chunks,)),
            dma((row_chunks,)),
            pltpu.VMEM((count, span), BF16),
            pltpu.VMEM((count, span), BF16),
            pltpu.VMEM((pieces, count, span), BF16),
            pltpu.VMEM((3, pieces, count, span), BF16),
            pltpu.VMEM((w_pieces, n, rows, span * pieces // w_pieces), BF16),
            pltpu.VMEM((n,) + wo.shape, BF16),
            pltpu.VMEM((4, n // 2, 2 * rows, count), F32),
            pltpu.VMEM((2, n, rows, count), BF16),
            pltpu.VMEM((2, n, rows, count), BF16),
            pltpu.VMEM((2, 2, n, qk_rows, count), BF16),
            pltpu.VMEM((n, qk_rows, 2 * count), BF16),
            pltpu.VMEM((n, rows, 2 * count), BF16),
            pltpu.VMEM((n, channels, feature_rows), BF16),
            pltpu.VMEM((n, channels, feature_rows), BF16),
            pltpu.VMEM((2, feature_rows, 2 * count), BF16),
            pltpu.VMEM((2, n, qk_rows, count), BF16),
            pltpu.VMEM((2, channels, 2 * count), F32),
            pltpu.VMEM((n, channels, count), BF16),
            pltpu.VMEM((n, 2, 2, channels, count), BF16),
            pltpu.VMEM((n, count, 2 * head_width), BF16),
            pltpu.VMEM((count, columns), F32),
            dma((n,)),
            dma((n, w_pieces)),
            dma((3, 4)),
            dma((3, row_chunks)),
            dma((3, row_chunks)),
            dma((3, 2)),
            dma((n,)),
            dma((n,)),
            dma((n, out_pieces)),
            dma((n,)),
            dma((n,)),
            dma((2, n // 2)),
            dma((2, n // 2)),
            dma((2, n // 2, 2)),
            dma((2, n // 2, 2)),
            dma((n // 2,)),
            dma((n // 2,)),
            dma((n // 2,)),
            dma((n // 2, 3)),
            dma((n // 2, 2, 2)),
            pltpu.SemaphoreType.REGULAR,
        ],
        compiler_params=pltpu.CompilerParams(
            collective_id=0, has_side_effects=True, vmem_limit_bytes=60 * 1024 * 1024
        ),
    )(tokens, norm_gain.reshape(1, -1), head_gain.reshape(1, -1), wo, *shards)


def per_device(sizes, tokens, norm_gain, w_query, w_key, w_value, head_gain, w_out):
    n, nf, ns = sizes
    shards = [w_query[0], w_key[0], w_value[0]]
    if any(shard.shape[0] % 8 for shard in shards):
        shards = [jnp.concatenate(shards, 0)]
    rows, width = sum(shard.shape[0] for shard in shards), tokens.shape[1]
    count = tokens.shape[0]
    qk_rows = w_query.shape[1] + w_key.shape[1]
    channels = w_value.shape[1]
    head_width, columns = w_out.shape[1], w_out.shape[2]
    pieces = max(1, 16 // n)
    out_pieces = max(1, 16 // n)
    wo = w_out.reshape(ns, out_pieces, head_width // out_pieces, columns)
    hbm = pl.BlockSpec(memory_space=pl.ANY)
    vmem = pl.BlockSpec(memory_space=pltpu.VMEM)
    dma = pltpu.SemaphoreType.DMA
    return pl.pallas_call(
        functools.partial(kernel, n, nf, ns, pieces, out_pieces, len(shards)),
        out_shape=jax.ShapeDtypeStruct((count, columns), BF16),
        in_specs=[hbm, vmem, vmem, hbm] + [hbm] * len(shards),
        out_specs=vmem,
        scratch_shapes=[
            pltpu.VMEM(tokens.shape, BF16),
            pltpu.VMEM((rows, width), BF16),
            pltpu.VMEM(wo.shape, BF16),
            dma((len(shards) + 2,)),
            pltpu.VMEM((2 * pieces, count, width // (2 * pieces)), BF16),
            pltpu.VMEM((n, 2, pieces, rows, width // (2 * pieces)), BF16),
            pltpu.VMEM((n,) + wo.shape, BF16),
            pltpu.VMEM((n, qk_rows, count), BF16),
            pltpu.VMEM((n, channels, count), BF16),
            pltpu.VMEM((n, nf, qk_rows, count), BF16),
            pltpu.VMEM((n, channels, count), BF16),
            pltpu.VMEM((n, nf * qk_rows // 2, count), BF16),
            pltpu.VMEM((n, nf * qk_rows // 2, count), BF16),
            pltpu.VMEM((n, channels, count), BF16),
            pltpu.VMEM((n, nf, ns, channels, count), BF16),
            pltpu.VMEM((n, count, ns * head_width), BF16),
            pltpu.VMEM((count, columns), F32),
        ]
        + [dma((n, pieces))] * 5
        + [dma((n, out_pieces))] * 5
        + [
            dma((n, nf)),
            dma((n, nf)),
            dma((n,)),
            dma((n,)),
            dma((n,)),
            dma((n,)),
            dma((n, nf, ns)),
            dma((n, nf, ns)),
        ],
        compiler_params=pltpu.CompilerParams(
            collective_id=0, has_side_effects=True, vmem_limit_bytes=60 * 1024 * 1024
        ),
    )(tokens, norm_gain.reshape(1, -1), head_gain.reshape(1, -1), wo, *shards)


def solution(mesh):
    in_specs = (
        P(("groups", "seq"), None),
        P(),
        P(("seq", "sub"), "fsdp", None),
        P(("seq", "sub"), "fsdp", None),
        P(("seq", "sub"), "fsdp", None),
        P(),
        P("seq", None, ("fsdp", "sub")),
    )
    out_specs = P(("groups", "seq"), ("fsdp", "sub"))
    sizes = (mesh.shape["seq"], mesh.shape["fsdp"], mesh.shape["sub"])
    if sizes == (4, 2, 2):
        body = functools.partial(per_device_line, sizes[0])
    else:
        body = functools.partial(per_device, sizes)
    return jax.shard_map(
        body,
        mesh=mesh,
        in_specs=in_specs,
        out_specs=out_specs,
        check_vma=False,
    )
```
